8 devices in a mesh: stage: 4 (over z, y, x), expert: 2 (over core).
Axes of the slice: x: 2, y: 2, z: 1, core: 2. Of those that a mesh axis runs over, the one named last changes fastest.
Arguments:
- w_gate: bfloat16 [8, 16, 1024, 512], P('stage', 'expert')
- w_up: bfloat16 [8, 16, 1024, 512], P('stage', 'expert')
- w_down: bfloat16 [8, 16, 512, 1024], P('stage', 'expert')
- hot_units: int32 [2], replicated
- slot_map: int32 [8, 2], replicated
Outputs:
- output 1: bfloat16 [8, 32, 1024, 1024], P(None, ('stage', 'expert'))
- output 2: bfloat16 [8, 32, 512, 1024], P(None, ('stage', 'expert'))
All inputs are finite; a program needn't handle non-finite values.
Results may differ from the reference program's by a relative error of at most 0.001.
Values are sent between devices in bfloat16 or wider.
A program may use at most 1 GiB of HBM per device.

```python
import jax
import jax.numpy as jnp

LAYERS = 8
EXPERTS = 16
D_MODEL = 1024
FF_EXPERT = 512
DEVICES_FLAT = 8
HOT_UNITS = 2
EXTRA_SLOTS = 2

SPLIT_COUNT = max(DEVICES_FLAT // EXPERTS, 1)
UNITS_DEV = max(EXPERTS // DEVICES_FLAT, 1)
FF_DEV = FF_EXPERT // SPLIT_COUNT
UNIT_COUNT = EXPERTS * SPLIT_COUNT
SLOTS_DEV = UNITS_DEV + EXTRA_SLOTS
REPLICAS = 3 * DEVICES_FLAT // 2


def setup_inputs(seed: int = 0) -> dict:
    base_key = jax.random.key(seed)
    key_gate, key_up, key_down, key_hot, key_slot = jax.random.split(base_key, 5)
    gate_shape = (LAYERS, EXPERTS, D_MODEL, FF_EXPERT)
    down_shape = (LAYERS, EXPERTS, FF_EXPERT, D_MODEL)
    w_gate = (jax.random.normal(key_gate, gate_shape, jnp.float32) * D_MODEL ** -0.5).astype(jnp.bfloat16)
    w_up = (jax.random.normal(key_up, gate_shape, jnp.float32) * D_MODEL ** -0.5).astype(jnp.bfloat16)
    w_down = (jax.random.normal(key_down, down_shape, jnp.float32) * FF_EXPERT ** -0.5).astype(jnp.bfloat16)
    hot_units = jax.random.permutation(key_hot, UNIT_COUNT)[:HOT_UNITS].astype(jnp.int32)
    slot_order = jax.random.permutation(key_slot, DEVICES_FLAT * EXTRA_SLOTS)
    slot_map = jnp.where(slot_order < REPLICAS, slot_order % HOT_UNITS, -1).astype(jnp.int32).reshape(DEVICES_FLAT, EXTRA_SLOTS)
    return {'w_gate': w_gate, 'w_up': w_up, 'w_down': w_down, 'hot_units': hot_units, 'slot_map': slot_map}


def reference(w_gate, w_up, w_down, hot_units, slot_map):
    gate_parts = w_gate.reshape(LAYERS, EXPERTS, D_MODEL, SPLIT_COUNT, FF_DEV)
    up_parts = w_up.reshape(LAYERS, EXPERTS, D_MODEL, SPLIT_COUNT, FF_DEV)
    fused_units = jnp.concatenate([gate_parts, up_parts], axis=-1).transpose(0, 1, 3, 2, 4).reshape(LAYERS, UNIT_COUNT, D_MODEL, 2 * FF_DEV)
    down_units = w_down.reshape(LAYERS, UNIT_COUNT, FF_DEV, D_MODEL)
    slot_used = slot_map >= 0
    extra_ids = jnp.where(slot_used, hot_units[jnp.maximum(slot_map, 0)], 0).reshape(-1)
    keep_mask = slot_used.reshape(1, DEVICES_FLAT, EXTRA_SLOTS, 1, 1)
    fused_extra = jnp.where(keep_mask, jnp.take(fused_units, extra_ids, axis=1).reshape(LAYERS, DEVICES_FLAT, EXTRA_SLOTS, D_MODEL, 2 * FF_DEV), 0)
    down_extra = jnp.where(keep_mask, jnp.take(down_units, extra_ids, axis=1).reshape(LAYERS, DEVICES_FLAT, EXTRA_SLOTS, FF_DEV, D_MODEL), 0)
    fused_home = fused_units.reshape(LAYERS, DEVICES_FLAT, UNITS_DEV, D_MODEL, 2 * FF_DEV)
    down_home = down_units.reshape(LAYERS, DEVICES_FLAT, UNITS_DEV, FF_DEV, D_MODEL)
    w13 = jnp.concatenate([fused_home, fused_extra], axis=2).reshape(LAYERS, DEVICES_FLAT * SLOTS_DEV, D_MODEL, 2 * FF_DEV)
    w_down_out = jnp.concatenate([down_home, down_extra], axis=2).reshape(LAYERS, DEVICES_FLAT * SLOTS_DEV, FF_DEV, D_MODEL)
    return w13, w_down_out
```

```python
import functools

import jax
import jax.numpy as jnp
from jax import lax
from jax.experimental import pallas as pl
from jax.experimental.pallas import tpu as pltpu
from jax.sharding import PartitionSpec as P

MESH = pl.DeviceIdType.MESH
ANY = pl.BlockSpec(memory_space=pl.ANY)
SMEM = pl.BlockSpec(memory_space=pltpu.SMEM)
BF16 = jnp.bfloat16
LAYERS, LOCAL_LAYERS, LOCAL_EXPERTS, HIDDEN, WIDTH = 8, 2, 8, 1024, 512
SLOTS, HOME, HOT = 4, 2, 2


def coords():
    stage, core = lax.axis_index('stage'), lax.axis_index('expert')
    return stage, core, stage // 2, stage % 2


def pick_kernel(hot_ref, gate, up, down, fused_out, down_out, vf, vd, sem):
    core = lax.axis_index('expert')
    for h in range(HOT):
        unit = hot_ref[h]

        @pl.when(unit // LOCAL_EXPERTS == core)
        def _():
            e = unit % LOCAL_EXPERTS
            ins, outs = [], []
            for a in range(LOCAL_LAYERS):
                ins.append([
                    pltpu.make_async_copy(gate.at[a, e], vf.at[a, :, pl.ds(0, WIDTH)], sem.at[a, 0]),
                    pltpu.make_async_copy(up.at[a, e], vf.at[a, :, pl.ds(WIDTH, WIDTH)], sem.at[a, 1]),
                    pltpu.make_async_copy(down.at[a, e], vd.at[a], sem.at[a, 2])])
                outs.append([
                    pltpu.make_async_copy(vf.at[a], fused_out.at[h, a], sem.at[a, 3]),
                    pltpu.make_async_copy(vd.at[a], down_out.at[h, a], sem.at[a, 4])])
            for group in ins:
                for c in group:
                    c.start()
            for group, out in zip(ins, outs):
                for c in group:
                    c.wait()
                for c in out:
                    c.start()
            for out in outs:
                for c in out:
                    c.wait()


def exchange_kernel(owners, gate, up, down, fused_cand, down_cand, fused_home, down_home, fused_hot, down_hot,
                    send_home, recv_home, send_hot, recv_hot, send_peer, recv_peer):
    stage, core, y, x = coords()
    ops = (gate, up, down)

    def to(xx, yy, cc):
        return (yy * 2 + xx, cc)

    def home_copies(q, cc, near):
        e0 = q * 4 + cc * 2
        rows, units = pl.ds(2 * stage, 2), pl.ds(e0, 2)
        dsts = (fused_home.at[rows, :, :, pl.ds(0, WIDTH)], fused_home.at[rows, :, :, pl.ds(WIDTH, WIDTH)], down_home.at[rows])
        return [pltpu.make_async_remote_copy(
            src_ref=ops[k].at[:, units], dst_ref=dsts[k], send_sem=send_home.at[near, cc, k],
            recv_sem=recv_home.at[stage, k], device_id=to(q, core, cc), device_id_type=MESH) for k in range(3)]

    def hot_copies(h, a, origin, slot, device, sslot):
        layer = 2 * origin + a
        own = slot is None
        srcs = (fused_cand.at[h, a], down_cand.at[h, a]) if own else (fused_hot.at[h, layer], down_hot.at[h, layer])
        dsts = (fused_hot.at[h, layer], down_hot.at[h, layer])
        return srcs, dsts, layer

    def remote(srcs, dsts, ss, rs, device):
        return [pltpu.make_async_remote_copy(src_ref=srcs[k], dst_ref=dsts[k], send_sem=ss.at[k], recv_sem=rs.at[k],
                                             device_id=device, device_id_type=MESH) for k in range(2)]

    xn, yn = to(1 - x, y, core), to(x, 1 - y, core)
    x_stage, y_stage, d_stage = y * 2 + (1 - x), (1 - y) * 2 + x, (1 - y) * 2 + (1 - x)

    def hot_own(h, a):
        return (fused_cand.at[h, a], down_cand.at[h, a])

    def hot_at(h, layer):
        return (fused_hot.at[h, layer], down_hot.at[h, layer])

    def start(copies):
        for c in copies:
            c.start()

    own_sends, forwards, peer = {}, {}, {}
    for h in range(HOT):
        for a in range(2):
            dst = hot_at(h, 2 * stage + a)
            own_sends[h, a] = (remote(hot_own(h, a), dst, send_hot.at[h, a, 0], recv_hot.at[h, a, 0], xn),
                               remote(hot_own(h, a), dst, send_hot.at[h, a, 1], recv_hot.at[h, a, 1], yn))
            via = x_stage if a == 0 else y_stage
            piece = hot_at(h, 2 * via + a)
            forwards[h, a] = remote(piece, piece, send_hot.at[h, a, 2], recv_hot.at[h, a, 2], yn if a == 0 else xn)
            for r, origin in enumerate((stage, x_stage, y_stage, d_stage)):
                piece = hot_at(h, 2 * origin + a)
                peer[h, a, r] = remote(hot_own(h, a) if r == 0 else piece, piece, send_peer.at[h, a, r], recv_peer.at[h, a, r],
                                       (stage, 1 - core))

    def arrived(h, a, r):
        origin = (stage, x_stage, y_stage, d_stage)[r]
        piece = hot_at(h, 2 * origin + a)
        return remote(piece, piece, send_hot.at[h, a, r - 1], recv_hot.at[h, a, r - 1], xn)

    for h in range(HOT):
        @pl.when(core == owners[h])
        def _():
            for a in range(2):
                for group in own_sends[h, a]:
                    start(group)
                start(peer[h, a, 0])

    for cc in range(2):
        @pl.when(jnp.logical_or(core != y, core != cc))
        def _():
            start(home_copies(x, cc, 0))
    for cc in range(2):
        start(home_copies(1 - x, cc, 1))

    for h in range(HOT):
        @pl.when(core == owners[h])
        def _():
            for a in range(2):
                for c in arrived(h, a, a + 1):
                    c.wait_recv()
                start(forwards[h, a])
                start(peer[h, a, a + 1])
            for a in range(2):
                for c in arrived(h, a, 2 - a):
                    c.wait_recv()
                start(peer[h, a, 2 - a])
    for h in range(HOT):
        @pl.when(core == owners[h])
        def _():
            for a in range(2):
                for c in arrived(h, a, 3):
                    c.wait_recv()
                start(peer[h, a, 3])

    for h in range(HOT):
        @pl.when(core == owners[h])
        def _():
            for a in range(2):
                for group in (*own_sends[h, a], forwards[h, a]):
                    for c in group:
                        c.wait_send()
                for r in range(4):
                    for c in peer[h, a, r]:
                        c.wait_send()

        @pl.when(core != owners[h])
        def _():
            for a in range(2):
                for r in range(4):
                    for c in peer[h, a, r]:
                        c.wait_recv()
    for near, q in ((0, x), (1, 1 - x)):
        for cc in range(2):
            def waits():
                for c in home_copies(q, cc, near):
                    c.wait_send()
            if near == 0:
                pl.when(jnp.logical_or(core != y, core != cc))(waits)
            else:
                waits()
    for s in range(4):
        @pl.when(jnp.logical_or(s != stage, core != y))
        def _():
            rows = pl.ds(2 * s, 2)
            dsts = (fused_home.at[rows, :, :, pl.ds(0, WIDTH)], fused_home.at[rows, :, :, pl.ds(WIDTH, WIDTH)], down_home.at[rows])
            for k in range(3):
                pltpu.make_async_remote_copy(
                    src_ref=dsts[k], dst_ref=dsts[k], send_sem=send_home.at[0, 0, k], recv_sem=recv_home.at[s, k],
                    device_id=xn, device_id_type=MESH).wait_recv()


DEPTH, LAG = 10, 5


def place_kernel(hot_ref, map_ref, gate, up, down, fused_cand, down_cand, fused_home, down_home, fused_hot, down_hot,
                 fused_out, down_out, vf, vd, zf, zd, in_sem, out_sem, zero_sem):
    stage, core, y, x = coords()
    flat = stage * 2 + core
    zf[...] = jnp.zeros_like(zf)
    zd[...] = jnp.zeros_like(zd)
    items = [(l, t) for t in range(SLOTS) for l in range(LAYERS)]

    def inputs(k):
        l, t = items[k]
        b = k % DEPTH
        bf, bd = vf.at[b], vd.at[b]
        own = stage == l // 2
        if t < HOME:
            whole = lambda f, d: [pltpu.make_async_copy(f, bf, in_sem.at[b, 0]), pltpu.make_async_copy(d, bd, in_sem.at[b, 1])]
            e = x * 4 + core * 2 + t
            a = l % 2
            direct = jnp.logical_and(own, core == y)
            parts = [pltpu.make_async_copy(gate.at[a, e], bf.at[:, pl.ds(0, WIDTH)], in_sem.at[b, 0]),
                     pltpu.make_async_copy(up.at[a, e], bf.at[:, pl.ds(WIDTH, WIDTH)], in_sem.at[b, 2]),
                     pltpu.make_async_copy(down.at[a, e], bd, in_sem.at[b, 1])]
            return [(direct, parts), (jnp.logical_not(direct), whole(fused_home.at[l, t], down_home.at[l, t]))]
        h = map_ref[flat, t - HOME]
        used = h >= 0
        hh = jnp.maximum(h, 0)
        direct = jnp.logical_and(own, hot_ref[hh] // LOCAL_EXPERTS == core)
        copies = lambda f, d: [pltpu.make_async_copy(f, bf, in_sem.at[b, 0]), pltpu.make_async_copy(d, bd, in_sem.at[b, 1])]
        return [(jnp.logical_and(used, direct), copies(fused_cand.at[hh, l % 2], down_cand.at[hh, l % 2])),
                (jnp.logical_and(used, jnp.logical_not(direct)), copies(fused_hot.at[hh, l], down_hot.at[hh, l]))]

    def outputs(k):
        l, t = items[k]
        b = k % DEPTH
        put = [pltpu.make_async_copy(vf.at[b], fused_out.at[l, t], out_sem.at[b, 0]),
               pltpu.make_async_copy(vd.at[b], down_out.at[l, t], out_sem.at[b, 1])]
        if t < HOME:
            return [(None, put)]
        used = map_ref[flat, t - HOME] >= 0
        zero = [pltpu.make_async_copy(zf, fused_out.at[l, t], out_sem.at[b, 0]),
                pltpu.make_async_copy(zd, down_out.at[l, t], out_sem.at[b, 1])]
        return [(used, put), (jnp.logical_not(used), zero)]

    def run(groups, verb):
        for cond, copies in groups:
            def act():
                for c in copies:
                    getattr(c, verb)()
            if cond is None:
                act()
            else:
                pl.when(cond)(act)

    n = len(items)
    for k in range(n + LAG):
        if k < n:
            if k >= DEPTH:
                run(outputs(k - DEPTH)[:1] if items[k - DEPTH][1] < HOME else outputs(k - DEPTH), 'wait')
            run(inputs(k), 'start')
        if k >= LAG:
            run(inputs(k - LAG), 'wait')
            run(outputs(k - LAG), 'start')
    for k in range(n - DEPTH, n):
        run(outputs(k), 'wait')


def solution(mesh):
    flat_axes = ('stage', 'expert')
    S = jax.ShapeDtypeStruct
    cand = (S((HOT, LOCAL_LAYERS, HIDDEN, 2 * WIDTH), BF16), S((HOT, LOCAL_LAYERS, WIDTH, HIDDEN), BF16))
    home = (S((LAYERS, HOME, HIDDEN, 2 * WIDTH), BF16), S((LAYERS, HOME, WIDTH, HIDDEN), BF16))
    hot = (S((HOT, LAYERS, HIDDEN, 2 * WIDTH), BF16), S((HOT, LAYERS, WIDTH, HIDDEN), BF16))
    outs = (S((LAYERS, SLOTS, HIDDEN, 2 * WIDTH), BF16), S((LAYERS, SLOTS, WIDTH, HIDDEN), BF16))
    DMA = pltpu.SemaphoreType.DMA

    pick = pl.pallas_call(
        pick_kernel, out_shape=cand, in_specs=[SMEM, ANY, ANY, ANY], out_specs=(ANY, ANY),
        scratch_shapes=[pltpu.VMEM((LOCAL_LAYERS, HIDDEN, 2 * WIDTH), BF16), pltpu.VMEM((LOCAL_LAYERS, WIDTH, HIDDEN), BF16),
                        DMA((LOCAL_LAYERS, 5))])

    def exchange(owners):
        return pl.pallas_call(
            functools.partial(exchange_kernel, owners), out_shape=(*home, *hot), in_specs=[ANY] * 5, out_specs=(ANY,) * 4,
            scratch_shapes=[DMA((2, 2, 3)), DMA((4, 3)), DMA((HOT, 2, 3, 2)), DMA((HOT, 2, 3, 2)),
                            DMA((HOT, 2, 4, 2)), DMA((HOT, 2, 4, 2))],
            compiler_params=pltpu.CompilerParams(has_side_effects=True))

    place = pl.pallas_call(
        place_kernel, out_shape=outs, in_specs=[SMEM, SMEM] + [ANY] * 9, out_specs=(ANY, ANY),
        scratch_shapes=[pltpu.VMEM((DEPTH, HIDDEN, 2 * WIDTH), BF16), pltpu.VMEM((DEPTH, WIDTH, HIDDEN), BF16),
                        pltpu.VMEM((HIDDEN, 2 * WIDTH), BF16), pltpu.VMEM((WIDTH, HIDDEN), BF16),
                        DMA((DEPTH, 3)), DMA((DEPTH, 2)), DMA((2,))],
        compiler_params=pltpu.CompilerParams(vmem_limit_bytes=48 * 1024 * 1024))

    def local(gate, up, down, hot_units, slot_map):
        fused_cand, down_cand = pick(hot_units, gate, up, down)
        owner = hot_units // LOCAL_EXPERTS
        received = lax.switch(owner[0] * 2 + owner[1], [exchange((a, b)) for a in range(2) for b in range(2)],
                              gate, up, down, fused_cand, down_cand)
        return place(hot_units, slot_map, gate, up, down, fused_cand, down_cand, *received)

    return jax.shard_map(local, mesh=mesh, in_specs=(P('stage', 'expert'), P('stage', 'expert'), P('stage', 'expert'), P(), P()),
                         out_specs=(P(None, flat_axes), P(None, flat_axes)), check_vma=False)
```

```python
import functools

import jax
import jax.numpy as jnp
from jax import lax
from jax.experimental import pallas as pl
from jax.experimental.pallas import tpu as pltpu
from jax.sharding import PartitionSpec as P

MESH = pl.DeviceIdType.MESH
ANY = pl.BlockSpec(memory_space=pl.ANY)
SMEM = pl.BlockSpec(memory_space=pltpu.SMEM)
BF16 = jnp.bfloat16
LAYERS, LOCAL_LAYERS, LOCAL_EXPERTS, HIDDEN, WIDTH = 8, 2, 8, 1024, 512
SLOTS, HOME, HOT = 4, 2, 2


def coords():
    stage, core = lax.axis_index('stage'), lax.axis_index('expert')
    return stage, core, stage // 2, stage % 2


def unit_reads(gate, up, down, a, e, dst, sem):
    return [pltpu.make_async_copy(gate.at[a, e], dst.at[pl.ds(0, HIDDEN), pl.ds(0, WIDTH)], sem.at[0]),
            pltpu.make_async_copy(up.at[a, e], dst.at[pl.ds(0, HIDDEN), pl.ds(WIDTH, WIDTH)], sem.at[1]),
            pltpu.make_async_copy(down.at[a, e], dst.at[pl.ds(HIDDEN, WIDTH)], sem.at[2])]


def pick_kernel(hot_ref, gate, up, down, cand, vm, sem):
    core = lax.axis_index('expert')
    for h in range(HOT):
        unit = hot_ref[h]

        @pl.when(unit // LOCAL_EXPERTS == core)
        def _():
            e = unit % LOCAL_EXPERTS
            ins = [unit_reads(gate, up, down, a, e, vm.at[h, a], sem.at[h, a]) for a in range(LOCAL_LAYERS)]
            outs = [pltpu.make_async_copy(vm.at[h, a], cand.at[h, a], sem.at[h, a, 3]) for a in range(LOCAL_LAYERS)]
            for group in ins:
                for c in group:
                    c.start()
            for group, out in zip(ins, outs):
                for c in group:
                    c.wait()
                out.start()
            for out in outs:
                out.wait()


def exchange_kernel(owners, gate, up, down, cand, fused_home, down_home, hot, late,
                    send_home, recv_home, send_hot, recv_hot, send_peer, recv_peer, vm, late_sem):
    stage, core, y, x = coords()
    ops = (gate, up, down)
    x_stage, y_stage, d_stage = y * 2 + (1 - x), (1 - y) * 2 + x, (1 - y) * 2 + (1 - x)
    xn, yn = (x_stage, core), (y_stage, core)

    def start(copies):
        for c in copies:
            c.start()

    def home_dsts(s, t0, count):
        rows, units = pl.ds(2 * s, 2), pl.ds(t0, count)
        return (fused_home.at[rows, units, :, pl.ds(0, WIDTH)], fused_home.at[rows, units, :, pl.ds(WIDTH, WIDTH)],
                down_home.at[rows, units])

    def home_copies(far, cc, t0):
        q = 1 - x if far else x
        dsts = home_dsts(stage, t0, 2 - t0)
        return [pltpu.make_async_remote_copy(
            src_ref=ops[k].at[:, pl.ds(q * 4 + cc * 2 + t0, 2 - t0)], dst_ref=dsts[k], send_sem=send_home.at[far, cc, k],
            recv_sem=recv_home.at[stage, k], device_id=(core * 2 + q, cc), device_id_type=MESH) for k in range(3)]

    def each_home(far, act):
        if far:
            act(home_copies(1, 1, 0))
            pl.when(core != y)(lambda: act(home_copies(1, 0, 0)))
            pl.when(core == y)(lambda: act(home_copies(1, 0, 1)))
        else:
            pl.when(core != y)(lambda: act(home_copies(0, 0, 0) + home_copies(0, 1, 1)))
            pl.when(jnp.logical_and(core == y, core == 0))(lambda: act(home_copies(0, 1, 0)))
            pl.when(jnp.logical_and(core == y, core == 1))(lambda: act(home_copies(0, 0, 0)))

    def remote(src, dst, ss, rs, device):
        return pltpu.make_async_remote_copy(src_ref=src, dst_ref=dst, send_sem=ss, recv_sem=rs, device_id=device,
                                            device_id_type=MESH)

    own_sends, forwards, peer = {}, {}, {}
    for h in range(HOT):
        for a in range(2):
            mine, dst = cand.at[h, a], hot.at[h, 2 * stage + a]
            own_sends[h, a] = (remote(mine, dst, send_hot.at[h, a, 0], recv_hot.at[h, a, 0], xn),
                               remote(mine, dst, send_hot.at[h, a, 1], recv_hot.at[h, a, 1], yn))
            piece = hot.at[h, 2 * (x_stage if a == 0 else y_stage) + a]
            forwards[h, a] = remote(piece, piece, send_hot.at[h, a, 2], recv_hot.at[h, a, 2], yn if a == 0 else xn)
            for r, origin in enumerate((stage, x_stage, y_stage, d_stage)):
                piece = hot.at[h, 2 * origin + a]
                peer[h, a, r] = remote(mine if r == 0 else piece, piece, send_peer.at[h, a, r], recv_peer.at[h, a, r],
                                       (stage, 1 - core))

    def arrival(h, a, r):
        piece = hot.at[h, 2 * (stage, x_stage, y_stage, d_stage)[r] + a]
        return remote(piece, piece, send_hot.at[h, a, r - 1], recv_hot.at[h, a, r - 1], xn)

    for h in range(HOT):
        @pl.when(core == owners[h])
        def _():
            for a in range(2):
                start(own_sends[h, a])
                peer[h, a, 0].start()

    each_home(0, start)
    each_home(1, start)

    late_unit = jnp.where(core == y, (1 - x) * 4, x * 4 + 2)
    reads = [unit_reads(gate, up, down, a, late_unit, vm.at[a], late_sem.at[a]) for a in range(2)]
    writes = [pltpu.make_async_copy(vm.at[a], late.at[a], late_sem.at[a, 3]) for a in range(2)]
    for group in reads:
        start(group)
    for group, write in zip(reads, writes):
        for c in group:
            c.wait()
        write.start()
    for write in writes:
        write.wait()

    for h in range(HOT):
        @pl.when(core == owners[h])
        def _():
            for a in range(2):
                arrival(h, a, a + 1).wait_recv()
                forwards[h, a].start()
                peer[h, a, a + 1].start()
            for a in range(2):
                arrival(h, a, 2 - a).wait_recv()
                peer[h, a, 2 - a].start()
    for h in range(HOT):
        @pl.when(core == owners[h])
        def _():
            for a in range(2):
                arrival(h, a, 3).wait_recv()
                peer[h, a, 3].start()

    for h in range(HOT):
        @pl.when(core == owners[h])
        def _():
            for a in range(2):
                for c in (*own_sends[h, a], forwards[h, a], *(peer[h, a, r] for r in range(4))):
                    c.wait_send()

        @pl.when(core != owners[h])
        def _():
            for a in range(2):
                for r in range(4):
                    peer[h, a, r].wait_recv()

    def sent(copies):
        for c in copies:
            c.wait_send()

    each_home(0, sent)
    each_home(1, sent)
    late_stage = jnp.where(core == 0, x_stage, y_stage)
    for s in range(4):
        def received(t0):
            for k, dst in enumerate(home_dsts(s, t0, 2 - t0)):
                remote(dst, dst, send_home.at[0, 0, k], recv_home.at[s, k], xn).wait_recv()

        pl.when(s == late_stage)(lambda: received(1))
        pl.when(jnp.logical_and(s != late_stage, jnp.logical_or(s != stage, core != y)))(lambda: received(0))


DEPTH, LAG = 10, 5


def place_kernel(hot_ref, map_ref, gate, up, down, cand, fused_home, down_home, hot,
                 fused_out, down_out, vm, zero, in_sem, out_sem):
    stage, core, y, x = coords()
    flat = stage * 2 + core
    late_stage = jnp.where(core == 0, y * 2 + (1 - x), (1 - y) * 2 + x)
    zero[...] = jnp.zeros_like(zero)
    items = [(l, t) for t in range(SLOTS) for l in range(LAYERS)]

    def inputs(k):
        l, t = items[k]
        b = k % DEPTH
        bf, bd = vm.at[b, pl.ds(0, HIDDEN)], vm.at[b, pl.ds(HIDDEN, WIDTH)]
        own = stage == l // 2
        if t < HOME:
            e = x * 4 + core * 2 + t
            direct = jnp.logical_and(own, core == y)
            arrived = [pltpu.make_async_copy(fused_home.at[l, t], bf, in_sem.at[b, 0]),
                       pltpu.make_async_copy(down_home.at[l, t], bd, in_sem.at[b, 1])]
            other = jnp.logical_not(direct)
            if t == 0:
                other = jnp.logical_and(other, late_stage != l // 2)
            return [(direct, unit_reads(gate, up, down, l % 2, e, vm.at[b], in_sem.at[b])), (other, arrived)]
        h = map_ref[flat, t - HOME]
        used = h >= 0
        hh = jnp.maximum(h, 0)
        direct = jnp.logical_and(own, hot_ref[hh] // LOCAL_EXPERTS == core)
        return [(jnp.logical_and(used, direct), [pltpu.make_async_copy(cand.at[hh, l % 2], vm.at[b], in_sem.at[b, 0])]),
                (jnp.logical_and(used, jnp.logical_not(direct)), [pltpu.make_async_copy(hot.at[hh, l], vm.at[b], in_sem.at[b, 0])])]

    def outputs(k):
        l, t = items[k]
        b = k % DEPTH

        def put(src):
            return [pltpu.make_async_copy(src.at[pl.ds(0, HIDDEN)], fused_out.at[l, t], out_sem.at[b, 0]),
                    pltpu.make_async_copy(src.at[pl.ds(HIDDEN, WIDTH)], down_out.at[l, t], out_sem.at[b, 1])]
        if t == 0:
            return [(late_stage != l // 2, put(vm.at[b]))]
        if t < HOME:
            return [(None, put(vm.at[b]))]
        used = map_ref[flat, t - HOME] >= 0
        return [(used, put(vm.at[b])), (jnp.logical_not(used), put(zero))]

    def run(groups, verb):
        for cond, copies in groups:
            def act():
                for c in copies:
                    getattr(c, verb)()
            if cond is None:
                act()
            else:
                pl.when(cond)(act)

    n = len(items)
    for k in range(n + LAG):
        if k < n:
            if k >= DEPTH:
                run(outputs(k - DEPTH), 'wait')
            run(inputs(k), 'start')
        if k >= LAG:
            run(inputs(k - LAG), 'wait')
            run(outputs(k - LAG), 'start')
    for k in range(n - DEPTH, n):
        run(outputs(k), 'wait')


def finish_kernel(late, fused_in, down_in, fused_out, down_out, vm, sem):
    del fused_in, down_in
    stage, core, y, x = coords()
    late_stage = jnp.where(core == 0, y * 2 + (1 - x), (1 - y) * 2 + x)
    reads = [pltpu.make_async_copy(late.at[a], vm.at[a], sem.at[a, 0]) for a in range(2)]
    for c in reads:
        c.start()
    writes = []
    for a in range(2):
        reads[a].wait()
        l = 2 * late_stage + a
        for c in (pltpu.make_async_copy(vm.at[a, pl.ds(0, HIDDEN)], fused_out.at[l, 0], sem.at[a, 1]),
                  pltpu.make_async_copy(vm.at[a, pl.ds(HIDDEN, WIDTH)], down_out.at[l, 0], sem.at[a, 2])):
            c.start()
            writes.append(c)
    for c in writes:
        c.wait()


def solution(mesh):
    flat_axes = ('stage', 'expert')
    S = jax.ShapeDtypeStruct
    ROWS = HIDDEN + WIDTH
    home = (S((LAYERS, HOME, HIDDEN, 2 * WIDTH), BF16), S((LAYERS, HOME, WIDTH, HIDDEN), BF16))
    outs = (S((LAYERS, SLOTS, HIDDEN, 2 * WIDTH), BF16), S((LAYERS, SLOTS, WIDTH, HIDDEN), BF16))
    DMA = pltpu.SemaphoreType.DMA

    pick = pl.pallas_call(
        pick_kernel, out_shape=S((HOT, LOCAL_LAYERS, ROWS, HIDDEN), BF16), in_specs=[SMEM, ANY, ANY, ANY], out_specs=ANY,
        scratch_shapes=[pltpu.VMEM((HOT, LOCAL_LAYERS, ROWS, HIDDEN), BF16), DMA((HOT, LOCAL_LAYERS, 4))])

    def exchange(owners):
        return pl.pallas_call(
            functools.partial(exchange_kernel, owners),
            out_shape=(*home, S((HOT, LAYERS, ROWS, HIDDEN), BF16), S((LOCAL_LAYERS, ROWS, HIDDEN), BF16)),
            in_specs=[ANY] * 4, out_specs=(ANY,) * 4,
            scratch_shapes=[DMA((2, 2, 3)), DMA((4, 3)), DMA((HOT, 2, 3)), DMA((HOT, 2, 3)), DMA((HOT, 2, 4)), DMA((HOT, 2, 4)),
                            pltpu.VMEM((LOCAL_LAYERS, ROWS, HIDDEN), BF16), DMA((LOCAL_LAYERS, 4))],
            compiler_params=pltpu.CompilerParams(has_side_effects=True))

    place = pl.pallas_call(
        place_kernel, out_shape=outs, in_specs=[SMEM, SMEM] + [ANY] * 7, out_specs=(ANY, ANY),
        scratch_shapes=[pltpu.VMEM((DEPTH, ROWS, HIDDEN), BF16), pltpu.VMEM((ROWS, HIDDEN), BF16), DMA((DEPTH, 3)), DMA((DEPTH, 2))],
        cost_estimate=pl.CostEstimate(flops=10 ** 9, bytes_accessed=2 * 10 ** 8, transcendentals=0),
        compiler_params=pltpu.CompilerParams(vmem_limit_bytes=48 * 1024 * 1024))

    finish = pl.pallas_call(
        finish_kernel, out_shape=outs, in_specs=[ANY] * 3, out_specs=(ANY, ANY), input_output_aliases={1: 0, 2: 1},
        scratch_shapes=[pltpu.VMEM((LOCAL_LAYERS, ROWS, HIDDEN), BF16), DMA((LOCAL_LAYERS, 3))])

    pairs = []
    for y in range(2):
        for x in range(2):
            pairs.append(((y * 2 + x) * 2 + y, (y * 2 + 1 - x) * 2))
            pairs.append(((y * 2 + x) * 2 + 1 - y, ((1 - y) * 2 + x) * 2 + 1))

    def local(gate, up, down, hot_units, slot_map):
        cand = pick(hot_units, gate, up, down)
        owner = hot_units // LOCAL_EXPERTS
        fused_home, down_home, hot, late = lax.switch(
            owner[0] * 2 + owner[1], [exchange((a, b)) for a in range(2) for b in range(2)], gate, up, down, cand)
        late = lax.ppermute(late, flat_axes, pairs)
        fused, down_out = place(hot_units, slot_map, gate, up, down, cand, fused_home, down_home, hot)
        return finish(late, fused, down_out)

    return jax.shard_map(local, mesh=mesh, in_specs=(P('stage', 'expert'), P('stage', 'expert'), P('stage', 'expert'), P(), P()),
                         out_specs=(P(None, flat_axes), P(None, flat_axes)), check_vma=False)
```

```python
import functools

import jax
import jax.numpy as jnp
from jax import lax
from jax.experimental import pallas as pl
from jax.experimental.pallas import tpu as pltpu
from jax.sharding import PartitionSpec as P

MESH = pl.DeviceIdType.MESH
ANY = pl.BlockSpec(memory_space=pl.ANY)
SMEM = pl.BlockSpec(memory_space=pltpu.SMEM)
BF16 = jnp.bfloat16
LAYERS, LOCAL_LAYERS, LOCAL_EXPERTS, HIDDEN, WIDTH = 8, 2, 8, 1024, 512
SLOTS, HOME, HOT = 4, 2, 2
ROWS = HIDDEN + WIDTH
ROW_STEPS = ROWS // 16


def coords():
    stage, core = lax.axis_index('stage'), lax.axis_index('expert')
    return stage, core, stage // 2, stage % 2


def unit_reads(gate, up, down, a, e, dst, sem):
    return [pltpu.make_async_copy(gate.at[a, e], dst.at[pl.ds(0, HIDDEN), pl.ds(0, WIDTH)], sem.at[0]),
            pltpu.make_async_copy(up.at[a, e], dst.at[pl.ds(0, HIDDEN), pl.ds(WIDTH, WIDTH)], sem.at[1]),
            pltpu.make_async_copy(down.at[a, e], dst.at[pl.ds(HIDDEN, WIDTH)], sem.at[2])]


X_FIRST = {0: ((0, 0, 2, 0), (2, 0, 2, 0)), 1: ((0, 0, 2, 2), (0, 0, 2, 2)), 2: ((2, 0, 2, 0), (2, 0, 2, 0)), 3: ((0, 0, 0, 0), (1, 1, 1, 1))}
Y_FIRST = {0: (2, 1, 3, 0), 1: (0, 0, 2, 2), 2: (4, 0, 4, 0), 3: (0, 0, 0, 0)}
PAIRS = [(n0, n1) for n1 in range(8) for n0 in range(n1 + 1)]


def by_stage(stage, values):
    if len(set(values)) == 1:
        return values[0]
    return sum(jnp.where(stage == i, v, 0) for i, v in enumerate(values))


def exchange_kernel(homes, hot_ref, gate, up, down, fused_home, down_home, hot, late, transit,
                    send_home, recv_home, send_hot, recv_hot, send_peer, recv_peer, send_part, send_fwd, recv_fwd,
                    pair_vm, pair_sem, late_vm, late_sem):
    stage, core, y, x = coords()
    ops = (gate, up, down)
    x_stage, y_stage, d_stage = y * 2 + (1 - x), (1 - y) * 2 + x, (1 - y) * 2 + (1 - x)
    xn, yn, mate = (x_stage, core), (y_stage, core), (stage, 1 - core)
    twin = homes[0] == homes[1]
    chips, owners = [n // 2 for n in homes], [n // 4 for n in homes]
    diff = chips[0] ^ chips[1]
    x_first = [[X_FIRST[diff][h][c ^ chips[0]] for c in range(4)] for h in range(HOT)]
    y_first = [Y_FIRST[diff][c ^ chips[0]] for c in range(4)]
    free_core = [next((cc for cc in range(2) if (3 - c) * 2 + cc not in homes), 0) for c in range(4)]

    def both(*conds):
        out = conds[0]
        for c in conds[1:]:
            out = jnp.logical_and(out, c)
        return out

    def is_hot_home(n):
        return jnp.logical_or(n == homes[0], n == homes[1])

    def start(copies):
        for c in copies:
            c.start()

    def remote(src, dst, ss, rs, device):
        return pltpu.make_async_remote_copy(src_ref=src, dst_ref=dst, send_sem=ss, recv_sem=rs, device_id=device,
                                            device_id_type=MESH)

    def split_dsts(s, t, a):
        l = 2 * s + a
        return (fused_home.at[l, t, :, pl.ds(0, WIDTH)], fused_home.at[l, t, :, pl.ds(WIDTH, WIDTH)], down_home.at[l, t])

    def packed_dsts(s, t, a):
        return (fused_home.at[2 * s + a, t], down_home.at[2 * s + a, t])

    def packed_sems(s, t, a):
        return (recv_home.at[s, t, a, 0], recv_home.at[s, t, a, 2])

    def flipped(source, cc, t, a):
        rank = (1 - t) * 2 + a
        return both(cc == by_stage(source, free_core), rank < by_stage(source, y_first))

    def home_piece(far, cc, t, a):
        q = x + far * (1 - 2 * x)
        home = (core * 2 + q) * 2 + cc
        e = q * 4 + cc * 2 + t
        p = ((far * 2 + cc) * 2 + t) * 2 + a
        mine = both(far == 0, core == y, core == cc)
        held = both(t == 0, jnp.where(core == y, both(far == 1, cc == 0), both(far == 0, cc == 1)))
        turned = both(core != y, far == 1, flipped(stage, cc, t, a))
        send = both(jnp.logical_not(mine), jnp.logical_not(held), jnp.logical_not(is_hot_home(home)))
        dsts, buffer = split_dsts(stage, t, a), transit.at[(1 - t) * 2 + a]
        bufs = (buffer.at[pl.ds(0, HIDDEN), pl.ds(0, WIDTH)], buffer.at[pl.ds(0, HIDDEN), pl.ds(WIDTH, WIDTH)],
                buffer.at[pl.ds(HIDDEN, WIDTH)])
        direct = [remote(ops[k].at[a, e], dsts[k], send_home.at[p, k], recv_home.at[stage, t, a, k], (core * 2 + q, cc)) for k in range(3)]
        round_about = [remote(ops[k].at[a, e], bufs[k], send_home.at[p, k], recv_fwd.at[(1 - t) * 2 + a, k], yn) for k in range(3)]
        return both(send, jnp.logical_not(turned)), direct, both(send, turned), round_about

    def home_pieces(lo, hi, verb, turn):
        def step(i, carry):
            a, far, cc, t = i % 2, 1 - (i // 2) % 2, 1 - (i // 4) % 2, 1 - i // 8
            straight_on, direct, turned, round_about = home_piece(far, cc, t, a)
            for on, copies, this in ((straight_on, direct, False), (turned, round_about, True)):
                if turn is None or turn == this:
                    @pl.when(on)
                    def _():
                        for c in copies:
                            getattr(c, verb)()
            return carry
        lax.fori_loop(lo, hi, step, 0)

    def pair_reads(h):
        units = pl.ds(2 * (homes[h] % 4), 2)
        dst = pair_vm.at[h]
        return [pltpu.make_async_copy(gate.at[:, units], dst.at[:, :, pl.ds(0, HIDDEN), pl.ds(0, WIDTH)], pair_sem.at[h, 0]),
                pltpu.make_async_copy(up.at[:, units], dst.at[:, :, pl.ds(0, HIDDEN), pl.ds(WIDTH, WIDTH)], pair_sem.at[h, 1]),
                pltpu.make_async_copy(down.at[:, units], dst.at[:, :, pl.ds(HIDDEN, WIDTH)], pair_sem.at[h, 2])]

    held_home = jnp.where(core == y, x_stage * 2, y_stage * 2 + 1)
    held_unit = jnp.where(core == y, (1 - x) * 4, x * 4 + 2)
    loads = HOT if not twin else 1
    for h in range(loads):
        @pl.when(core == owners[h])
        def _():
            start(pair_reads(h))
    held_reads = [unit_reads(gate, up, down, a, held_unit, late_vm.at[a], late_sem.at[a]) for a in range(2)]
    for group in held_reads:
        start(group)

    home_pieces(0, 16, 'start', True)
    home_pieces(0, 4, 'start', False)

    for h in range(loads):
        @pl.when(core == owners[h])
        def _():
            for c in pair_reads(h):
                c.wait()
            if not twin:
                first, second = hot_ref[0], hot_ref[1]
                unit = jnp.minimum(first, second) if h == 0 else jnp.maximum(first, second)
                odd = jnp.full((16, HIDDEN), unit % 2, jnp.int32) == 1

                def swap(i, carry):
                    a, rows = i // ROW_STEPS, pl.ds(pl.multiple_of((i % ROW_STEPS) * 16, 16), 16)
                    one, two = pair_vm[h, a, 0, rows, :], pair_vm[h, a, 1, rows, :]
                    pair_vm[h, a, 0, rows, :] = jnp.where(odd, two, one)
                    pair_vm[h, a, 1, rows, :] = jnp.where(odd, one, two)
                    return carry
                lax.fori_loop(0, 2 * ROW_STEPS, swap, 0, unroll=4)
    for group in held_reads:
        for c in group:
            c.wait()

    def own(h, a):
        return pair_vm.at[0, a, h] if twin else pair_vm.at[h, a, 0]

    first_hop = {(h, a): (remote(own(h, a), hot.at[h, 2 * stage + a], send_hot.at[h, a, 0], recv_hot.at[h, a, 0], xn),
                          remote(own(h, a), hot.at[h, 2 * stage + a], send_hot.at[h, a, 1], recv_hot.at[h, a, 1], yn))
                 for h in range(HOT) for a in range(2)}

    def onward(h, a):
        out = []
        for r, origin, device in ((0, x_stage, yn), (1, y_stage, xn)):
            goes = by_stage(origin, [int(x_first[h][c] > a) == 1 - r for c in range(4)])
            goes = goes if isinstance(goes, bool) else goes == 1
            piece = hot.at[h, 2 * origin + a]
            out.append((goes, remote(piece, piece, send_hot.at[h, a, 2 + r], recv_hot.at[h, a, 2], device)))
        return out

    def to_mate(h, a, r):
        piece = hot.at[h, 2 * (stage, x_stage, y_stage, d_stage)[r] + a]
        return remote(own(h, a) if r == 0 else piece, piece, send_peer.at[h, a, r], recv_peer.at[h, a, r], mate)

    def arrival(h, a, r):
        piece = hot.at[h, 2 * (x_stage, y_stage, d_stage)[r] + a]
        return remote(piece, piece, send_hot.at[h, a, r], recv_hot.at[h, a, r], xn)

    def partner(h, a):
        dsts, sems, src = packed_dsts(stage, 1, a), packed_sems(stage, 1, a), pair_vm.at[h, a, 1]
        device = (chips[h], homes[h] % 2)
        return [remote(src.at[pl.ds(0, HIDDEN)], dsts[0], send_part.at[h, a, 0], sems[0], device),
                remote(src.at[pl.ds(HIDDEN, WIDTH)], dsts[1], send_part.at[h, a, 1], sems[1], device)]

    def partner_sent(h):
        return both(core == owners[h], held_home != homes[h],
                    jnp.logical_not(both(stage == chips[h], owners[h] == homes[h] % 2)))

    held_write = [[pltpu.make_async_copy(src, late.at[a], late_sem.at[a, 3]) for a, src in enumerate(srcs)]
                  for srcs in ([late_vm.at[0], late_vm.at[1]], *([[pair_vm.at[h, 0, 1], pair_vm.at[h, 1, 1]] for h in range(loads)]))]
    if twin:
        held_write = held_write[:1]
    from_pair = [held_home == homes[h] for h in range(HOT)] if not twin else []
    regular = jnp.logical_not(is_hot_home(held_home)) if not twin else None

    for h in range(HOT):
        @pl.when(core == owners[h])
        def _():
            for a in range(2):
                start(first_hop[h, a])
            for a in range(2):
                to_mate(h, a, 0).start()
    if twin:
        start(held_write[0])
    else:
        pl.when(regular)(lambda: start(held_write[0]))
        for h in range(HOT):
            pl.when(from_pair[h])(lambda: start(held_write[1 + h]))
            pl.when(partner_sent(h))(lambda: start(partner(h, 0) + partner(h, 1)))

    ahead = 16 if diff == 1 else 8
    home_pieces(4, ahead, 'start', False)

    turns = max(y_first)

    def turned_in(p, act):
        t, a = 1 - p // 2, p % 2
        cc = by_stage(y_stage, free_core)
        buffer = transit.at[p]
        bufs = (buffer.at[pl.ds(0, HIDDEN), pl.ds(0, WIDTH)], buffer.at[pl.ds(0, HIDDEN), pl.ds(WIDTH, WIDTH)],
                buffer.at[pl.ds(HIDDEN, WIDTH)])
        incoming = [remote(b, b, send_home.at[0, k], recv_fwd.at[p, k], yn) for k, b in enumerate(bufs)]
        dsts, sems = packed_dsts(y_stage, t, a), packed_sems(y_stage, t, a)
        srcs = (buffer.at[pl.ds(0, HIDDEN)], buffer.at[pl.ds(HIDDEN, WIDTH)])
        leaving = [remote(srcs[k], dsts[k], send_fwd.at[p, k], sems[k], (x_stage, cc)) for k in range(2)]
        pl.when(both(core == y, p < by_stage(y_stage, y_first)))(lambda: act(incoming, leaving))

    def pass_on(incoming, leaving):
        for c in incoming:
            c.wait_recv()
        start(leaving)

    for p in range(turns):
        turned_in(p, pass_on)

    for a in range(2):
        for h in range(HOT):
            @pl.when(core == owners[h])
            def _():
                for r, (goes, c) in enumerate(onward(h, a)):
                    arrival(h, a, r).wait_recv()
                    pl.when(goes)(lambda: c.start())
                    to_mate(h, a, r + 1).start()

    home_pieces(ahead, 16, 'start', False)

    for a in range(2):
        for h in range(HOT):
            @pl.when(core == owners[h])
            def _():
                arrival(h, a, 2).wait_recv()
                to_mate(h, a, 3).start()

    for h in range(HOT):
        @pl.when(core == owners[h])
        def _():
            for a in range(2):
                for c in first_hop[h, a]:
                    c.wait_send()
                for goes, c in onward(h, a):
                    pl.when(goes)(lambda: c.wait_send())
                for r in range(4):
                    to_mate(h, a, r).wait_send()

        @pl.when(core != owners[h])
        def _():
            for a in range(2):
                for r in range(4):
                    to_mate(h, a, r).wait_recv()
    if twin:
        for c in held_write[0]:
            c.wait()
    else:
        def wait_write(i):
            for c in held_write[i]:
                c.wait()

        def wait_sent(h):
            for c in partner(h, 0) + partner(h, 1):
                c.wait_send()

        pl.when(regular)(lambda: wait_write(0))
        for h in range(HOT):
            pl.when(from_pair[h])(lambda: wait_write(1 + h))
            pl.when(partner_sent(h))(lambda: wait_sent(h))

    def left(incoming, leaving):
        for c in leaving:
            c.wait_send()

    for p in range(turns):
        turned_in(p, left)
    home_pieces(0, 16, 'wait_send', None)

    late_stage = jnp.where(core == 0, x_stage, y_stage)
    home = stage * 2 + core

    def receive(i, carry):
        s, t, a = i // 4, (i // 2) % 2, i % 2
        away = jnp.logical_or(s != stage, core != y)
        in_hot = is_hot_home(home)
        diagonal = s == d_stage
        packed = both(diagonal, flipped(s, core, t, a))
        plain = both(away, jnp.logical_not(in_hot), jnp.logical_not(both(s == late_stage, t == 0)))

        def arrived(dsts, sems):
            for dst, sem in zip(dsts, sems):
                remote(dst, dst, send_home.at[0, 0], sem, xn).wait_recv()

        pl.when(both(plain, jnp.logical_not(packed)))(
            lambda: arrived(split_dsts(s, t, a), [recv_home.at[s, t, a, k] for k in range(3)]))
        whole = both(plain, packed)
        if not twin:
            whole = jnp.logical_or(whole, both(away, in_hot, s != late_stage, t == 1))
        pl.when(whole)(lambda: arrived(packed_dsts(s, t, a), packed_sems(s, t, a)))
        return carry

    lax.fori_loop(0, 16, receive, 0)


def hot_facts(hot_ref, flat):
    low, high = jnp.minimum(hot_ref[0], hot_ref[1]), jnp.maximum(hot_ref[0], hot_ref[1])
    at_low, at_high = low // HOME == flat, high // HOME == flat
    one = at_low != at_high
    hot_place = jnp.where(at_low, low, high) % HOME
    late_place = jnp.where(one, 1 - hot_place, 0)
    return low, high, one, late_place


DEPTH, LAG = 10, 5


def place_kernel(hot_ref, map_ref, gate, up, down, fused_home, down_home, hot,
                 fused_out, down_out, vm, zero, in_sem, out_sem):
    stage, core, y, x = coords()
    flat = stage * 2 + core
    late_stage = jnp.where(core == 0, y * 2 + (1 - x), (1 - y) * 2 + x)
    low, high, one_hot, late_place = hot_facts(hot_ref, flat)
    crossed = (hot_ref[0] > hot_ref[1]).astype(jnp.int32)
    zero[...] = jnp.zeros_like(zero)
    items = [(l, t) for t in range(SLOTS) for l in range(LAYERS)]

    def is_late(l, t):
        return jnp.logical_and(late_stage == l // 2, late_place == t)

    def inputs(k):
        l, t = items[k]
        b = k % DEPTH
        bf, bd = vm.at[b, pl.ds(0, HIDDEN)], vm.at[b, pl.ds(HIDDEN, WIDTH)]
        own = stage == l // 2
        if t < HOME:
            unit = flat * HOME + t
            hot_here = jnp.logical_or(unit == low, unit == high)
            h = (unit == high).astype(jnp.int32)
            direct = jnp.logical_and(own, core == y)
            other = jnp.logical_not(jnp.logical_or(direct, is_late(l, t)))
            place = jnp.where(one_hot, 1, t)
            arrived = [pltpu.make_async_copy(fused_home.at[l, place], bf, in_sem.at[b, 0]),
                       pltpu.make_async_copy(down_home.at[l, place], bd, in_sem.at[b, 1])]
            return [(direct, unit_reads(gate, up, down, l % 2, x * 4 + core * 2 + t, vm.at[b], in_sem.at[b])),
                    (jnp.logical_and(other, hot_here), [pltpu.make_async_copy(hot.at[h, l], vm.at[b], in_sem.at[b, 0])]),
                    (jnp.logical_and(other, jnp.logical_not(hot_here)), arrived)]
        v = map_ref[flat, t - HOME]
        used = v >= 0
        v = jnp.maximum(v, 0)
        unit = hot_ref[v]
        direct = jnp.logical_and(own, unit // LOCAL_EXPERTS == core)
        return [(jnp.logical_and(used, direct), unit_reads(gate, up, down, l % 2, unit % LOCAL_EXPERTS, vm.at[b], in_sem.at[b])),
                (jnp.logical_and(used, jnp.logical_not(direct)),
                 [pltpu.make_async_copy(hot.at[jnp.where(crossed == 1, 1 - v, v), l], vm.at[b], in_sem.at[b, 0])])]

    def outputs(k):
        l, t = items[k]
        b = k % DEPTH

        def put(src):
            return [pltpu.make_async_copy(src.at[pl.ds(0, HIDDEN)], fused_out.at[l, t], out_sem.at[b, 0]),
                    pltpu.make_async_copy(src.at[pl.ds(HIDDEN, WIDTH)], down_out.at[l, t], out_sem.at[b, 1])]
        if t < HOME:
            return [(jnp.logical_not(is_late(l, t)), put(vm.at[b]))]
        used = map_ref[flat, t - HOME] >= 0
        return [(used, put(vm.at[b])), (jnp.logical_not(used), put(zero))]

    def run(groups, verb):
        for cond, copies in groups:
            def act():
                for c in copies:
                    getattr(c, verb)()
            if cond is None:
                act()
            else:
                pl.when(cond)(act)

    n = len(items)
    for k in range(n + LAG):
        if k < n:
            if k >= DEPTH:
                run(outputs(k - DEPTH), 'wait')
            run(inputs(k), 'start')
        if k >= LAG:
            run(inputs(k - LAG), 'wait')
            run(outputs(k - LAG), 'start')
    for k in range(n - DEPTH, n):
        run(outputs(k), 'wait')


def finish_kernel(hot_ref, late, fused_in, down_in, fused_out, down_out, vm, sem):
    del fused_in, down_in
    stage, core, y, x = coords()
    late_stage = jnp.where(core == 0, y * 2 + (1 - x), (1 - y) * 2 + x)
    late_place = hot_facts(hot_ref, stage * 2 + core)[-1]
    reads = [pltpu.make_async_copy(late.at[a], vm.at[a], sem.at[a, 0]) for a in range(2)]
    for c in reads:
        c.start()
    writes = []
    for a in range(2):
        reads[a].wait()
        l = 2 * late_stage + a
        for c in (pltpu.make_async_copy(vm.at[a, pl.ds(0, HIDDEN)], fused_out.at[l, late_place], sem.at[a, 1]),
                  pltpu.make_async_copy(vm.at[a, pl.ds(HIDDEN, WIDTH)], down_out.at[l, late_place], sem.at[a, 2])):
            c.start()
            writes.append(c)
    for c in writes:
        c.wait()


def solution(mesh):
    flat_axes = ('stage', 'expert')
    S = jax.ShapeDtypeStruct
    home = (S((LAYERS, HOME, HIDDEN, 2 * WIDTH), BF16), S((LAYERS, HOME, WIDTH, HIDDEN), BF16))
    outs = (S((LAYERS, SLOTS, HIDDEN, 2 * WIDTH), BF16), S((LAYERS, SLOTS, WIDTH, HIDDEN), BF16))
    DMA = pltpu.SemaphoreType.DMA

    def exchange(homes):
        return pl.pallas_call(
            functools.partial(exchange_kernel, homes),
            out_shape=(*home, S((HOT, LAYERS, ROWS, HIDDEN), BF16), S((LOCAL_LAYERS, ROWS, HIDDEN), BF16), S((4, ROWS, HIDDEN), BF16)),
            in_specs=[SMEM] + [ANY] * 3, out_specs=(ANY,) * 5,
            scratch_shapes=[DMA((16, 3)), DMA((4, 2, 2, 3)), DMA((HOT, 2, 4)), DMA((HOT, 2, 3)), DMA((HOT, 2, 4)), DMA((HOT, 2, 4)),
                            DMA((HOT, 2, 2)), DMA((4, 2)), DMA((4, 3)),
                            pltpu.VMEM((HOT, LOCAL_LAYERS, 2, ROWS, HIDDEN), BF16), DMA((HOT, 3)),
                            pltpu.VMEM((LOCAL_LAYERS, ROWS, HIDDEN), BF16), DMA((LOCAL_LAYERS, 4))],
            compiler_params=pltpu.CompilerParams(has_side_effects=True, vmem_limit_bytes=48 * 1024 * 1024))

    place = pl.pallas_call(
        place_kernel, out_shape=outs, in_specs=[SMEM, SMEM] + [ANY] * 6, out_specs=(ANY, ANY),
        scratch_shapes=[pltpu.VMEM((DEPTH, ROWS, HIDDEN), BF16), pltpu.VMEM((ROWS, HIDDEN), BF16), DMA((DEPTH, 3)), DMA((DEPTH, 2))],
        cost_estimate=pl.CostEstimate(flops=10 ** 9, bytes_accessed=2 * 10 ** 8, transcendentals=0),
        compiler_params=pltpu.CompilerParams(vmem_limit_bytes=48 * 1024 * 1024))

    finish = pl.pallas_call(
        finish_kernel, out_shape=outs, in_specs=[SMEM] + [ANY] * 3, out_specs=(ANY, ANY), input_output_aliases={2: 0, 3: 1},
        scratch_shapes=[pltpu.VMEM((LOCAL_LAYERS, ROWS, HIDDEN), BF16), DMA((LOCAL_LAYERS, 3))])

    pairs = []
    for y in range(2):
        for x in range(2):
            pairs.append(((y * 2 + x) * 2 + y, (y * 2 + 1 - x) * 2))
            pairs.append(((y * 2 + x) * 2 + 1 - y, ((1 - y) * 2 + x) * 2 + 1))

    def local(gate, up, down, hot_units, slot_map):
        homes = hot_units // HOME
        low, high = jnp.min(homes), jnp.max(homes)
        fused_home, down_home, hot, late, _ = lax.switch(
            high * (high + 1) // 2 + low, [exchange(p) for p in PAIRS], hot_units, gate, up, down)
        late = lax.ppermute(late, flat_axes, pairs)
        fused, down_out = place(hot_units, slot_map, gate, up, down, fused_home, down_home, hot)
        return finish(hot_units, late, fused, down_out)

    return jax.shard_map(local, mesh=mesh, in_specs=(P('stage', 'expert'), P('stage', 'expert'), P('stage', 'expert'), P(), P()),
                         out_specs=(P(None, flat_axes), P(None, flat_axes)), check_vma=False)
```

```python
import functools

import jax
import jax.numpy as jnp
from jax import lax
from jax.experimental import pallas as pl
from jax.experimental.pallas import tpu as pltpu
from jax.sharding import PartitionSpec as P

MESH = pl.DeviceIdType.MESH
ANY = pl.BlockSpec(memory_space=pl.ANY)
SMEM = pl.BlockSpec(memory_space=pltpu.SMEM)
BF16 = jnp.bfloat16
LAYERS, LOCAL_LAYERS, LOCAL_EXPERTS, HIDDEN, WIDTH = 8, 2, 8, 1024, 512
SLOTS, HOME, HOT = 4, 2, 2
ROWS = HIDDEN + WIDTH
ROW_STEPS = ROWS // 16


def coords():
    stage, core = lax.axis_index('stage'), lax.axis_index('expert')
    return stage, core, stage // 2, stage % 2


def unit_reads(gate, up, down, a, e, dst, sem):
    return [pltpu.make_async_copy(gate.at[a, e], dst.at[pl.ds(0, HIDDEN), pl.ds(0, WIDTH)], sem.at[0]),
            pltpu.make_async_copy(up.at[a, e], dst.at[pl.ds(0, HIDDEN), pl.ds(WIDTH, WIDTH)], sem.at[1]),
            pltpu.make_async_copy(down.at[a, e], dst.at[pl.ds(HIDDEN, WIDTH)], sem.at[2])]


X_FIRST = {0: ((0, 0, 2, 0), (2, 0, 2, 0)), 1: ((0, 0, 2, 2), (0, 0, 2, 2)), 2: ((2, 0, 2, 0), (2, 0, 2, 0)), 3: ((0, 0, 0, 0), (1, 1, 1, 1))}
Y_FIRST = {0: (2, 1, 3, 0), 1: (0, 0, 2, 2), 2: (4, 0, 4, 0), 3: (0, 0, 0, 0)}
FIRST = {0: 4, 1: 4, 2: 4, 3: 4}
AHEAD = {0: 8, 1: 16, 2: 8, 3: 8}
PAIRS = [(n0, n1) for n1 in range(8) for n0 in range(n1 + 1)]


def by_stage(stage, values):
    if len(set(values)) == 1:
        return values[0]
    return sum(jnp.where(stage == i, v, 0) for i, v in enumerate(values))


def exchange_kernel(homes, hot_ref, gate, up, down, fused_home, down_home, hot, late, transit,
                    send_home, recv_home, send_hot, recv_hot, recv_peer, send_part, send_fwd, recv_fwd,
                    pair_vm, pair_sem, late_vm, late_sem):
    stage, core, y, x = coords()
    ops = (gate, up, down)
    x_stage, y_stage, d_stage = y * 2 + (1 - x), (1 - y) * 2 + x, (1 - y) * 2 + (1 - x)
    xn, yn, mate = (x_stage, core), (y_stage, core), (stage, 1 - core)
    twin = homes[0] == homes[1]
    chips, owners = [n // 2 for n in homes], [n // 4 for n in homes]
    diff = chips[0] ^ chips[1]
    x_first = [X_FIRST[diff][h][c ^ chips[0]] for h in range(HOT) for c in range(4)]
    y_first = [Y_FIRST[diff][c ^ chips[0]] for c in range(4)]
    free_core = [next((cc for cc in range(2) if (3 - c) * 2 + cc not in homes), 0) for c in range(4)]
    sizes = (pl.ds(0, HIDDEN), pl.ds(HIDDEN, WIDTH))

    def both(*conds):
        out = conds[0]
        for c in conds[1:]:
            out = jnp.logical_and(out, c)
        return out

    def no(cond):
        return jnp.logical_not(cond)

    def is_hot_home(n):
        return jnp.logical_or(n == homes[0], n == homes[1])

    def start(copies):
        for c in copies:
            c.start()

    def remote(src, dst, ss, rs, device):
        return pltpu.make_async_remote_copy(src_ref=src, dst_ref=dst, send_sem=ss, recv_sem=rs, device_id=device,
                                            device_id_type=MESH)

    piece_bytes = transit.at[0]

    def wait_for(sem, dst=piece_bytes):
        remote(dst, dst, send_home.at[0], sem, xn).wait_recv()

    def wait_left(sem, src=piece_bytes):
        remote(src, src, sem, recv_home.at[0, 0, 0], xn).wait_send()

    def split_dsts(s, t, a):
        l = 2 * s + a
        return (fused_home.at[l, t, :, pl.ds(0, WIDTH)], fused_home.at[l, t, :, pl.ds(WIDTH, WIDTH)], down_home.at[l, t])

    def packed_dsts(s, t, a):
        return (fused_home.at[2 * s + a, t], down_home.at[2 * s + a, t])

    def buffer_parts(p):
        part = transit.at[p]
        return (part.at[sizes[0], pl.ds(0, WIDTH)], part.at[sizes[0], pl.ds(WIDTH, WIDTH)], part.at[sizes[1]])

    def flipped(source, cc, t, a):
        return both(cc == by_stage(source, free_core), (1 - t) * 2 + a < by_stage(source, y_first))

    def home_piece(i):
        a, far, cc, t = i % 2, 1 - (i // 2) % 2, 1 - (i // 4) % 2, 1 - i // 8
        q = x + far * (1 - 2 * x)
        home = (core * 2 + q) * 2 + cc
        mine = both(far == 0, core == y, core == cc)
        held = both(t == 0, jnp.where(core == y, both(far == 1, cc == 0), both(far == 0, cc == 1)))
        turned = both(core != y, far == 1, flipped(stage, cc, t, a))
        send = both(no(mine), no(held), no(is_hot_home(home)))
        srcs = [ref.at[a, q * 4 + cc * 2 + t] for ref in ops]
        return a, t, (core * 2 + q, cc), srcs, send, turned

    def send_turned(i, carry):
        a, t, _, srcs, send, turned = home_piece(i)
        p = (1 - t) * 2 + a

        @pl.when(both(send, turned))
        def _():
            start([remote(srcs[k], dst, send_home.at[i], recv_fwd.at[p], yn) for k, dst in enumerate(buffer_parts(p))])
        return carry

    def send_straight(i, carry):
        a, t, device, srcs, send, turned = home_piece(i)

        @pl.when(both(send, no(turned)))
        def _():
            start([remote(srcs[k], dst, send_home.at[i], recv_home.at[stage, t, a], device)
                   for k, dst in enumerate(split_dsts(stage, t, a))])
        return carry

    def home_left(i, carry):
        send = home_piece(i)[4]

        pl.when(send)(lambda: wait_left(send_home.at[i]))
        return carry

    def owner(h):
        return owners[0] if owners[0] == owners[1] else jnp.where(h == 0, owners[0], owners[1])

    def home_of(h):
        return jnp.where(h == 0, homes[0], homes[1])

    def pair_reads(h):
        units = pl.ds(2 * (home_of(h) % 4), 2)
        dst = pair_vm.at[h]
        return [pltpu.make_async_copy(gate.at[:, units], dst.at[:, :, sizes[0], pl.ds(0, WIDTH)], pair_sem.at[h]),
                pltpu.make_async_copy(up.at[:, units], dst.at[:, :, sizes[0], pl.ds(WIDTH, WIDTH)], pair_sem.at[h]),
                pltpu.make_async_copy(down.at[:, units], dst.at[:, :, sizes[1]], pair_sem.at[h])]

    held_home = jnp.where(core == y, x_stage * 2, y_stage * 2 + 1)
    held_unit = jnp.where(core == y, (1 - x) * 4, x * 4 + 2)
    loads = 1 if twin else HOT

    def read_pair(h, carry):
        pl.when(core == owner(h))(lambda: start(pair_reads(h)))
        return carry

    def held_reads(a):
        return unit_reads(gate, up, down, a, held_unit, late_vm.at[a], late_sem.at[a])

    def read_held(a, carry):
        start(held_reads(a))
        return carry

    def await_held(a, carry):
        for c in held_reads(a):
            c.wait()
        return carry

    def order_pair(h, carry):
        @pl.when(core == owner(h))
        def _():
            pltpu.make_async_copy(pair_vm.at[h], pair_vm.at[h], pair_sem.at[h]).wait()
            if not twin:
                low, high = jnp.minimum(hot_ref[0], hot_ref[1]), jnp.maximum(hot_ref[0], hot_ref[1])
                unit = jnp.where(h == 0, low, high)
                odd = jnp.full((16, HIDDEN), unit % 2, jnp.int32) == 1

                def swap(i, inner):
                    a, rows = i // ROW_STEPS, pl.ds(pl.multiple_of((i % ROW_STEPS) * 16, 16), 16)
                    one, two = pair_vm[h, a, 0, rows, :], pair_vm[h, a, 1, rows, :]
                    pair_vm[h, a, 0, rows, :] = jnp.where(odd, two, one)
                    pair_vm[h, a, 1, rows, :] = jnp.where(odd, one, two)
                    return inner
                lax.fori_loop(0, 2 * ROW_STEPS, swap, 0)
        return carry

    def own(h, a):
        return pair_vm.at[0, a, h] if twin else pair_vm.at[h, a, 0]

    def send_hot_own(i, carry):
        h, a = i % 2, i // 2

        @pl.when(core == owner(h))
        def _():
            dst = hot.at[h, 2 * stage + a]
            start([remote(own(h, a), dst, send_hot.at[h, a, 0], recv_hot.at[h, a, 0], xn),
                   remote(own(h, a), dst, send_hot.at[h, a, 0], recv_hot.at[h, a, 1], yn),
                   remote(own(h, a), dst, send_hot.at[h, a, 0], recv_peer.at[h], mate)])
        return carry

    def goes_on(h, a, r):
        straight = by_stage(h * 4 + (x_stage, y_stage)[r], x_first) > a
        return straight if r == 0 else no(straight)

    def pass_hot(i, carry):
        h, a = i % 2, i // 2

        @pl.when(core == owner(h))
        def _():
            for r, origin, device in ((0, x_stage, yn), (1, y_stage, xn)):
                piece = hot.at[h, 2 * origin + a]
                wait_for(recv_hot.at[h, a, r])
                pl.when(goes_on(h, a, r))(
                    lambda: remote(piece, piece, send_hot.at[h, a, 1 + r], recv_hot.at[h, a, 2], device).start())
                remote(piece, piece, send_hot.at[h, a, 0], recv_peer.at[h], mate).start()
        return carry

    def pass_last(i, carry):
        h, a = i % 2, i // 2

        @pl.when(core == owner(h))
        def _():
            piece = hot.at[h, 2 * d_stage + a]
            wait_for(recv_hot.at[h, a, 2])
            remote(piece, piece, send_hot.at[h, a, 0], recv_peer.at[h], mate).start()
        return carry

    def hot_left(i, carry):
        h, a = i % 2, i // 2

        @pl.when(core == owner(h))
        def _():
            wait_left(send_hot.at[h, a, 0], hot.at[0, pl.ds(0, 6)])
            for r in range(2):
                pl.when(goes_on(h, a, r))(lambda: wait_left(send_hot.at[h, a, 1 + r]))
        return carry

    def hot_here(h, carry):
        pl.when(core != owner(h))(lambda: wait_for(recv_peer.at[h], hot.at[h]))
        return carry

    def partner_goes(h):
        n = home_of(h)
        return both(core == owner(h), held_home != n, no(both(stage == n // 2, core == n % 2)))

    def send_partner(i, carry):
        h, a = i % 2, i // 2

        @pl.when(partner_goes(h))
        def _():
            n, src = home_of(h), pair_vm.at[h, a, 1]
            dsts = packed_dsts(stage, 1, a)
            start([remote(src.at[sizes[k]], dsts[k], send_part.at[h, a], recv_home.at[stage, 1, a], (n // 2, n % 2))
                   for k in range(2)])
        return carry

    def partner_left(i, carry):
        h, a = i % 2, i // 2

        pl.when(partner_goes(h))(lambda: wait_left(send_part.at[h, a]))
        return carry

    def write_held(verb):
        def step(a, carry):
            def act(src):
                getattr(pltpu.make_async_copy(src, late.at[a], late_sem.at[a, 3]), verb)()
            if twin:
                act(late_vm.at[a])
            else:
                pl.when(no(is_hot_home(held_home)))(lambda: act(late_vm.at[a]))
                pl.when(is_hot_home(held_home))(lambda: act(pair_vm.at[jnp.where(held_home == homes[0], 0, 1), a, 1]))
            return carry
        return step

    turns = max(y_first)

    def turns_here(p):
        return both(core == y, p < by_stage(y_stage, y_first))

    def pass_turned(p, carry):
        @pl.when(turns_here(p))
        def _():
            wait_for(recv_fwd.at[p])
            t, a = 1 - p // 2, p % 2
            dsts = packed_dsts(y_stage, t, a)
            start([remote(transit.at[p, sizes[k]], dsts[k], send_fwd.at[p], recv_home.at[y_stage, t, a],
                          (x_stage, by_stage(y_stage, free_core))) for k in range(2)])
        return carry

    def turned_left(p, carry):
        pl.when(turns_here(p))(lambda: wait_left(send_fwd.at[p]))
        return carry

    late_stage = jnp.where(core == 0, x_stage, y_stage)
    home = stage * 2 + core

    def receive(i, carry):
        s, t, a = i // 4, (i // 2) % 2, i % 2
        away = jnp.logical_or(s != stage, core != y)
        in_hot = is_hot_home(home)
        comes = both(no(in_hot), no(both(s == late_stage, t == 0)))
        if not twin:
            comes = jnp.logical_or(comes, both(in_hot, s != late_stage, t == 1))
        pl.when(both(away, comes))(lambda: wait_for(recv_home.at[s, t, a]))
        return carry

    def loop(n, step):
        if n:
            lax.fori_loop(0, n, step, 0)

    loop(loads, read_pair)
    loop(2, read_held)
    if turns:
        loop(16, send_turned)
    first, ahead = FIRST[diff], AHEAD[diff]

    def phase(i, carry):
        lax.fori_loop(jnp.where(i == 0, 0, jnp.where(i == 1, first, ahead)), jnp.where(i == 0, first, jnp.where(i == 1, ahead, 16)),
                      send_straight, 0)

        @pl.when(i == 0)
        def _():
            loop(loads, order_pair)
            loop(2, await_held)
            loop(4, send_hot_own)
            if not twin:
                loop(4, send_partner)
            loop(2, write_held('start'))

        @pl.when(i == 1)
        def _():
            loop(turns, pass_turned)
            loop(4, pass_hot)
        return carry

    lax.fori_loop(0, 3, phase, 0)
    loop(4, pass_last)

    loop(4, hot_left)
    loop(2, hot_here)
    loop(2, write_held('wait'))
    if not twin:
        loop(4, partner_left)
    loop(turns, turned_left)
    loop(16, home_left)
    loop(16, receive)


def hot_facts(hot_ref, flat):
    low, high = jnp.minimum(hot_ref[0], hot_ref[1]), jnp.maximum(hot_ref[0], hot_ref[1])
    at_low, at_high = low // HOME == flat, high // HOME == flat
    one = at_low != at_high
    hot_place = jnp.where(at_low, low, high) % HOME
    late_place = jnp.where(one, 1 - hot_place, 0)
    return low, high, one, late_place


DEPTH, LAG = 10, 5


def place_kernel(hot_ref, map_ref, gate, up, down, fused_home, down_home, hot,
                 fused_out, down_out, vm, zero, in_sem, out_sem):
    stage, core, y, x = coords()
    flat = stage * 2 + core
    late_stage = jnp.where(core == 0, y * 2 + (1 - x), (1 - y) * 2 + x)
    low, high, one_hot, late_place = hot_facts(hot_ref, flat)
    crossed = (hot_ref[0] > hot_ref[1]).astype(jnp.int32)
    zero[...] = jnp.zeros_like(zero)
    items = [(l, t) for t in range(SLOTS) for l in range(LAYERS)]

    def is_late(l, t):
        return jnp.logical_and(late_stage == l // 2, late_place == t)

    def inputs(k):
        l, t = items[k]
        b = k % DEPTH
        bf, bd = vm.at[b, pl.ds(0, HIDDEN)], vm.at[b, pl.ds(HIDDEN, WIDTH)]
        own = stage == l // 2
        if t < HOME:
            unit = flat * HOME + t
            hot_here = jnp.logical_or(unit == low, unit == high)
            h = (unit == high).astype(jnp.int32)
            direct = jnp.logical_and(own, core == y)
            other = jnp.logical_not(jnp.logical_or(direct, is_late(l, t)))
            place = jnp.where(one_hot, 1, t)
            arrived = [pltpu.make_async_copy(fused_home.at[l, place], bf, in_sem.at[b, 0]),
                       pltpu.make_async_copy(down_home.at[l, place], bd, in_sem.at[b, 1])]
            return [(direct, unit_reads(gate, up, down, l % 2, x * 4 + core * 2 + t, vm.at[b], in_sem.at[b])),
                    (jnp.logical_and(other, hot_here), [pltpu.make_async_copy(hot.at[h, l], vm.at[b], in_sem.at[b, 0])]),
                    (jnp.logical_and(other, jnp.logical_not(hot_here)), arrived)]
        v = map_ref[flat, t - HOME]
        used = v >= 0
        v = jnp.maximum(v, 0)
        unit = hot_ref[v]
        direct = jnp.logical_and(own, unit // LOCAL_EXPERTS == core)
        return [(jnp.logical_and(used, direct), unit_reads(gate, up, down, l % 2, unit % LOCAL_EXPERTS, vm.at[b], in_sem.at[b])),
                (jnp.logical_and(used, jnp.logical_not(direct)),
                 [pltpu.make_async_copy(hot.at[jnp.where(crossed == 1, 1 - v, v), l], vm.at[b], in_sem.at[b, 0])])]

    def outputs(k):
        l, t = items[k]
        b = k % DEPTH

        def put(src):
            return [pltpu.make_async_copy(src.at[pl.ds(0, HIDDEN)], fused_out.at[l, t], out_sem.at[b, 0]),
                    pltpu.make_async_copy(src.at[pl.ds(HIDDEN, WIDTH)], down_out.at[l, t], out_sem.at[b, 1])]
        if t < HOME:
            return [(jnp.logical_not(is_late(l, t)), put(vm.at[b]))]
        used = map_ref[flat, t - HOME] >= 0
        return [(used, put(vm.at[b])), (jnp.logical_not(used), put(zero))]

    def run(groups, verb):
        for cond, copies in groups:
            def act():
                for c in copies:
                    getattr(c, verb)()
            if cond is None:
                act()
            else:
                pl.when(cond)(act)

    n = len(items)
    for k in range(n + LAG):
        if k < n:
            if k >= DEPTH:
                run(outputs(k - DEPTH), 'wait')
            run(inputs(k), 'start')
        if k >= LAG:
            run(inputs(k - LAG), 'wait')
            run(outputs(k - LAG), 'start')
    for k in range(n - DEPTH, n):
        run(outputs(k), 'wait')


def finish_kernel(hot_ref, late, fused_in, down_in, fused_out, down_out, vm, sem):
    del fused_in, down_in
    stage, core, y, x = coords()
    late_stage = jnp.where(core == 0, y * 2 + (1 - x), (1 - y) * 2 + x)
    late_place = hot_facts(hot_ref, stage * 2 + core)[-1]
    reads = [pltpu.make_async_copy(late.at[a], vm.at[a], sem.at[a, 0]) for a in range(2)]
    for c in reads:
        c.start()
    writes = []
    for a in range(2):
        reads[a].wait()
        l = 2 * late_stage + a
        for c in (pltpu.make_async_copy(vm.at[a, pl.ds(0, HIDDEN)], fused_out.at[l, late_place], sem.at[a, 1]),
                  pltpu.make_async_copy(vm.at[a, pl.ds(HIDDEN, WIDTH)], down_out.at[l, late_place], sem.at[a, 2])):
            c.start()
            writes.append(c)
    for c in writes:
        c.wait()


def solution(mesh):
    flat_axes = ('stage', 'expert')
    S = jax.ShapeDtypeStruct
    home = (S((LAYERS, HOME, HIDDEN, 2 * WIDTH), BF16), S((LAYERS, HOME, WIDTH, HIDDEN), BF16))
    outs = (S((LAYERS, SLOTS, HIDDEN, 2 * WIDTH), BF16), S((LAYERS, SLOTS, WIDTH, HIDDEN), BF16))
    DMA = pltpu.SemaphoreType.DMA

    def exchange(homes):
        return pl.pallas_call(
            functools.partial(exchange_kernel, homes),
            out_shape=(*home, S((HOT, LAYERS, ROWS, HIDDEN), BF16), S((LOCAL_LAYERS, ROWS, HIDDEN), BF16), S((4, ROWS, HIDDEN), BF16)),
            in_specs=[SMEM] + [ANY] * 3, out_specs=(ANY,) * 5,
            scratch_shapes=[DMA((16,)), DMA((4, 2, 2)), DMA((HOT, 2, 3)), DMA((HOT, 2, 3)), DMA((HOT,)), DMA((HOT, 2)), DMA((4,)), DMA((4,)),
                            pltpu.VMEM((HOT, LOCAL_LAYERS, 2, ROWS, HIDDEN), BF16), DMA((HOT,)),
                            pltpu.VMEM((LOCAL_LAYERS, ROWS, HIDDEN), BF16), DMA((LOCAL_LAYERS, 4))],
            compiler_params=pltpu.CompilerParams(has_side_effects=True, vmem_limit_bytes=48 * 1024 * 1024))

    place = pl.pallas_call(
        place_kernel, out_shape=outs, in_specs=[SMEM, SMEM] + [ANY] * 6, out_specs=(ANY, ANY),
        scratch_shapes=[pltpu.VMEM((DEPTH, ROWS, HIDDEN), BF16), pltpu.VMEM((ROWS, HIDDEN), BF16), DMA((DEPTH, 3)), DMA((DEPTH, 2))],
        cost_estimate=pl.CostEstimate(flops=10 ** 9, bytes_accessed=2 * 10 ** 8, transcendentals=0),
        compiler_params=pltpu.CompilerParams(vmem_limit_bytes=48 * 1024 * 1024))

    finish = pl.pallas_call(
        finish_kernel, out_shape=outs, in_specs=[SMEM] + [ANY] * 3, out_specs=(ANY, ANY), input_output_aliases={2: 0, 3: 1},
        scratch_shapes=[pltpu.VMEM((LOCAL_LAYERS, ROWS, HIDDEN), BF16), DMA((LOCAL_LAYERS, 3))])

    pairs = []
    for y in range(2):
        for x in range(2):
            pairs.append(((y * 2 + x) * 2 + y, (y * 2 + 1 - x) * 2))
            pairs.append(((y * 2 + x) * 2 + 1 - y, ((1 - y) * 2 + x) * 2 + 1))

    def local(gate, up, down, hot_units, slot_map):
        homes = hot_units // HOME
        low, high = jnp.min(homes), jnp.max(homes)
        fused_home, down_home, hot, late, _ = lax.switch(
            high * (high + 1) // 2 + low, [exchange(p) for p in PAIRS], hot_units, gate, up, down)
        late = lax.ppermute(late, flat_axes, pairs)
        fused, down_out = place(hot_units, slot_map, gate, up, down, fused_home, down_home, hot)
        return finish(hot_units, late, fused, down_out)

    return jax.shard_map(local, mesh=mesh, in_specs=(P('stage', 'expert'), P('stage', 'expert'), P('stage', 'expert'), P(), P()),
                         out_specs=(P(None, flat_axes), P(None, flat_axes)), check_vma=False)
```

```python
import functools

import jax
import jax.numpy as jnp
from jax import lax
from jax.experimental import pallas as pl
from jax.experimental.pallas import tpu as pltpu
from jax.sharding import PartitionSpec as P

MESH = pl.DeviceIdType.MESH
ANY = pl.BlockSpec(memory_space=pl.ANY)
SMEM = pl.BlockSpec(memory_space=pltpu.SMEM)
BF16 = jnp.bfloat16
LAYERS, LOCAL_LAYERS, LOCAL_EXPERTS, HIDDEN, WIDTH = 8, 2, 8, 1024, 512
SLOTS, HOME, HOT = 4, 2, 2
ROWS = HIDDEN + WIDTH
ROW_STEPS = ROWS // 16


def coords():
    stage, core = lax.axis_index('stage'), lax.axis_index('expert')
    return stage, core, stage // 2, stage % 2


def unit_reads(gate, up, down, a, e, dst, sem):
    return [pltpu.make_async_copy(gate.at[a, e], dst.at[pl.ds(0, HIDDEN), pl.ds(0, WIDTH)], sem.at[0]),
            pltpu.make_async_copy(up.at[a, e], dst.at[pl.ds(0, HIDDEN), pl.ds(WIDTH, WIDTH)], sem.at[1]),
            pltpu.make_async_copy(down.at[a, e], dst.at[pl.ds(HIDDEN, WIDTH)], sem.at[2])]


X_FIRST = {0: ((0, 0, 2, 0), (2, 0, 2, 0)), 1: ((0, 0, 2, 2), (0, 0, 2, 2)), 2: ((2, 0, 2, 0), (2, 0, 2, 0)), 3: ((0, 0, 0, 0), (1, 1, 1, 1))}
Y_FIRST = {0: (2, 1, 3, 0), 1: (0, 0, 2, 2), 2: (4, 0, 4, 0), 3: (0, 0, 0, 0)}
FIRST = {0: 4, 1: 4, 2: 4, 3: 4}
AHEAD = {0: 12, 1: 16, 2: 8, 3: 8}
PAIRS = [(n0, n1) for n1 in range(8) for n0 in range(n1 + 1)]


def by_stage(stage, values):
    if len(set(values)) == 1:
        return values[0]
    return sum(jnp.where(stage == i, v, 0) for i, v in enumerate(values))


def exchange_kernel(homes, hot_ref, gate, up, down, fused_home, down_home, hot, late, last, transit,
                    send_home, recv_home, send_hot, recv_hot, recv_peer, send_part, send_fwd, recv_fwd,
                    pair_vm, pair_sem, late_vm, late_sem, last_sem):
    stage, core, y, x = coords()
    ops = (gate, up, down)
    x_stage, y_stage, d_stage = y * 2 + (1 - x), (1 - y) * 2 + x, (1 - y) * 2 + (1 - x)
    xn, yn, mate = (x_stage, core), (y_stage, core), (stage, 1 - core)
    twin = homes[0] == homes[1]
    chips, owners = [n // 2 for n in homes], [n // 4 for n in homes]
    diff = chips[0] ^ chips[1]
    x_first = [X_FIRST[diff][h][c ^ chips[0]] for h in range(HOT) for c in range(4)]
    y_first = [Y_FIRST[diff][c ^ chips[0]] for c in range(4)]
    free_core = [next((cc for cc in range(2) if (3 - c) * 2 + cc not in homes), 0) for c in range(4)]
    sizes = (pl.ds(0, HIDDEN), pl.ds(HIDDEN, WIDTH))

    def both(*conds):
        out = conds[0]
        for c in conds[1:]:
            out = jnp.logical_and(out, c)
        return out

    def no(cond):
        return jnp.logical_not(cond)

    def is_hot_home(n):
        return jnp.logical_or(n == homes[0], n == homes[1])

    def start(copies):
        for c in copies:
            c.start()

    def remote(src, dst, ss, rs, device):
        return pltpu.make_async_remote_copy(src_ref=src, dst_ref=dst, send_sem=ss, recv_sem=rs, device_id=device,
                                            device_id_type=MESH)

    piece_bytes = transit.at[0]

    def wait_for(sem, dst=piece_bytes):
        remote(dst, dst, send_home.at[0], sem, xn).wait_recv()

    def wait_left(sem, src=piece_bytes):
        remote(src, src, sem, recv_home.at[0, 0, 0], xn).wait_send()

    def split_dsts(s, t, a):
        l = 2 * s + a
        return (fused_home.at[l, t, :, pl.ds(0, WIDTH)], fused_home.at[l, t, :, pl.ds(WIDTH, WIDTH)], down_home.at[l, t])

    def packed_dsts(s, t, a):
        return (fused_home.at[2 * s + a, t], down_home.at[2 * s + a, t])

    def buffer_parts(p):
        part = transit.at[p]
        return (part.at[sizes[0], pl.ds(0, WIDTH)], part.at[sizes[0], pl.ds(WIDTH, WIDTH)], part.at[sizes[1]])

    def flipped(source, cc, t, a):
        return both(cc == by_stage(source, free_core), (1 - t) * 2 + a < by_stage(source, y_first))

    def home_piece(i):
        a, far, cc, t = i % 2, 1 - (i // 2) % 2, 1 - (i // 4) % 2, 1 - i // 8
        q = x + far * (1 - 2 * x)
        home = (core * 2 + q) * 2 + cc
        mine = both(far == 0, core == y, core == cc)
        held = both(t == 0, jnp.where(core == y, both(far == 1, cc == 0), both(far == 0, cc == 1)))
        turned = both(core != y, far == 1, flipped(stage, cc, t, a))
        send = both(no(mine), no(held), no(is_hot_home(home)))
        srcs = [ref.at[a, q * 4 + cc * 2 + t] for ref in ops]
        return a, t, (core * 2 + q, cc), srcs, send, turned

    def send_turned(i, carry):
        a, t, _, srcs, send, turned = home_piece(i)
        p = (1 - t) * 2 + a

        @pl.when(both(send, turned))
        def _():
            start([remote(srcs[k], dst, send_home.at[i], recv_fwd.at[p], yn) for k, dst in enumerate(buffer_parts(p))])
        return carry

    def send_straight(i, carry):
        a, t, device, srcs, send, turned = home_piece(i)

        @pl.when(both(send, no(turned)))
        def _():
            start([remote(srcs[k], dst, send_home.at[i], recv_home.at[stage, t, a], device)
                   for k, dst in enumerate(split_dsts(stage, t, a))])
        return carry

    def home_left(i, carry):
        send = home_piece(i)[4]

        pl.when(send)(lambda: wait_left(send_home.at[i]))
        return carry

    def owner(h):
        return owners[0] if owners[0] == owners[1] else jnp.where(h == 0, owners[0], owners[1])

    def home_of(h):
        return jnp.where(h == 0, homes[0], homes[1])

    def pair_reads(h):
        units = pl.ds(2 * (home_of(h) % 4), 2)
        dst = pair_vm.at[h]
        return [pltpu.make_async_copy(gate.at[:, units], dst.at[:, :, sizes[0], pl.ds(0, WIDTH)], pair_sem.at[h]),
                pltpu.make_async_copy(up.at[:, units], dst.at[:, :, sizes[0], pl.ds(WIDTH, WIDTH)], pair_sem.at[h]),
                pltpu.make_async_copy(down.at[:, units], dst.at[:, :, sizes[1]], pair_sem.at[h])]

    held_home = jnp.where(core == y, x_stage * 2, y_stage * 2 + 1)
    held_unit = jnp.where(core == y, (1 - x) * 4, x * 4 + 2)
    loads = 1 if twin else HOT

    def read_pair(h, carry):
        pl.when(core == owner(h))(lambda: start(pair_reads(h)))
        return carry

    def held_reads(a):
        return unit_reads(gate, up, down, a, held_unit, late_vm.at[a], late_sem.at[a])

    def read_held(a, carry):
        start(held_reads(a))
        return carry

    def await_held(a, carry):
        for c in held_reads(a):
            c.wait()
        return carry

    def order_pair(h, carry):
        @pl.when(core == owner(h))
        def _():
            pltpu.make_async_copy(pair_vm.at[h], pair_vm.at[h], pair_sem.at[h]).wait()
            if not twin:
                low, high = jnp.minimum(hot_ref[0], hot_ref[1]), jnp.maximum(hot_ref[0], hot_ref[1])
                unit = jnp.where(h == 0, low, high)
                odd = jnp.full((16, HIDDEN), unit % 2, jnp.int32) == 1

                def swap(i, inner):
                    a, rows = i // ROW_STEPS, pl.ds(pl.multiple_of((i % ROW_STEPS) * 16, 16), 16)
                    one, two = pair_vm[h, a, 0, rows, :], pair_vm[h, a, 1, rows, :]
                    pair_vm[h, a, 0, rows, :] = jnp.where(odd, two, one)
                    pair_vm[h, a, 1, rows, :] = jnp.where(odd, one, two)
                    return inner
                lax.fori_loop(0, 2 * ROW_STEPS, swap, 0)
        return carry

    def own(h, a):
        return pair_vm.at[0, a, h] if twin else pair_vm.at[h, a, 0]

    def send_hot_own(i, carry):
        h, a = i % 2, i // 2

        @pl.when(core == owner(h))
        def _():
            dst = hot.at[h, 2 * stage + a]
            start([remote(own(h, a), dst, send_hot.at[h, a, 0], recv_hot.at[h, a, 0], xn),
                   remote(own(h, a), dst, send_hot.at[h, a, 0], recv_hot.at[h, a, 1], yn),
                   remote(own(h, a), dst, send_hot.at[h, a, 0], recv_peer.at[h], mate)])
        return carry

    def goes_on(h, a, r):
        straight = by_stage(h * 4 + (x_stage, y_stage)[r], x_first) > a
        return straight if r == 0 else no(straight)

    def pass_hot(i, carry):
        h, a = i % 2, i // 2

        @pl.when(core == owner(h))
        def _():
            for r, origin, device in ((0, x_stage, yn), (1, y_stage, xn)):
                piece = hot.at[h, 2 * origin + a]
                wait_for(recv_hot.at[h, a, r])
                pl.when(goes_on(h, a, r))(
                    lambda: remote(piece, piece, send_hot.at[h, a, 1 + r], recv_hot.at[h, a, 2], device).start())
                remote(piece, piece, send_hot.at[h, a, 0], recv_peer.at[h], mate).start()
        return carry

    def pass_last(i, carry):
        h, a = i % 2, i // 2

        @pl.when(core == owner(h))
        def _():
            piece = hot.at[h, 2 * d_stage + a]
            wait_for(recv_hot.at[h, a, 2])
            remote(piece, piece, send_hot.at[h, a, 0], recv_peer.at[h], mate).start()
        return carry

    def hot_left(i, carry):
        h, a = i % 2, i // 2

        @pl.when(core == owner(h))
        def _():
            wait_left(send_hot.at[h, a, 0], hot.at[0, pl.ds(0, 6)])
            for r in range(2):
                pl.when(goes_on(h, a, r))(lambda: wait_left(send_hot.at[h, a, 1 + r]))
        return carry

    def hot_here(h, carry):
        pl.when(core != owner(h))(lambda: wait_for(recv_peer.at[h], hot.at[h]))
        return carry

    def partner_goes(h):
        n = home_of(h)
        return both(core == owner(h), held_home != n, no(both(stage == n // 2, core == n % 2)))

    def send_partner(i, carry):
        h, a = i % 2, i // 2

        @pl.when(partner_goes(h))
        def _():
            n, src = home_of(h), pair_vm.at[h, a, 1]
            dsts = packed_dsts(stage, 1, a)
            start([remote(src.at[sizes[k]], dsts[k], send_part.at[h, a], recv_home.at[stage, 1, a], (n // 2, n % 2))
                   for k in range(2)])
        return carry

    def partner_left(i, carry):
        h, a = i % 2, i // 2

        pl.when(partner_goes(h))(lambda: wait_left(send_part.at[h, a]))
        return carry

    def write_held(verb):
        def act(src):
            for k, c in enumerate((pltpu.make_async_copy(src.at[0], late.at[pl.ds(0, ROWS)], late_sem.at[0, 3]),
                                   pltpu.make_async_copy(src.at[1, sizes[0]], late.at[pl.ds(ROWS, HIDDEN)], late_sem.at[1, 3]),
                                   pltpu.make_async_copy(src.at[1, sizes[1]], last, last_sem))):
                getattr(c, verb)()
        if twin:
            act(late_vm)
        else:
            pl.when(no(is_hot_home(held_home)))(lambda: act(late_vm))
            pl.when(is_hot_home(held_home))(lambda: act(pair_vm.at[jnp.where(held_home == homes[0], 0, 1), :, 1]))

    turns = max(y_first)

    def turns_here(p):
        return both(core == y, p < by_stage(y_stage, y_first))

    def pass_turned(p, carry):
        @pl.when(turns_here(p))
        def _():
            wait_for(recv_fwd.at[p])
            t, a = 1 - p // 2, p % 2
            dsts = packed_dsts(y_stage, t, a)
            start([remote(transit.at[p, sizes[k]], dsts[k], send_fwd.at[p], recv_home.at[y_stage, t, a],
                          (x_stage, by_stage(y_stage, free_core))) for k in range(2)])
        return carry

    def turned_left(p, carry):
        pl.when(turns_here(p))(lambda: wait_left(send_fwd.at[p]))
        return carry

    late_stage = jnp.where(core == 0, x_stage, y_stage)
    home = stage * 2 + core

    def receive(i, carry):
        s, t, a = i // 4, (i // 2) % 2, i % 2
        away = jnp.logical_or(s != stage, core != y)
        in_hot = is_hot_home(home)
        comes = both(no(in_hot), no(both(s == late_stage, t == 0)))
        if not twin:
            comes = jnp.logical_or(comes, both(in_hot, s != late_stage, t == 1))
        pl.when(both(away, comes))(lambda: wait_for(recv_home.at[s, t, a]))
        return carry

    def loop(n, step):
        if n:
            lax.fori_loop(0, n, step, 0)

    loop(loads, read_pair)
    loop(2, read_held)
    if turns:
        loop(16, send_turned)
    first, ahead = FIRST[diff], AHEAD[diff]

    def phase(i, carry):
        lax.fori_loop(jnp.where(i == 0, 0, jnp.where(i == 1, first, ahead)), jnp.where(i == 0, first, jnp.where(i == 1, ahead, 16)),
                      send_straight, 0)

        @pl.when(i == 0)
        def _():
            loop(loads, order_pair)
            loop(2, await_held)
            loop(4, send_hot_own)
            if not twin:
                loop(4, send_partner)
            write_held('start')

        @pl.when(i == 1)
        def _():
            loop(turns, pass_turned)
            loop(4, pass_hot)
        return carry

    lax.fori_loop(0, 3, phase, 0)
    loop(4, pass_last)

    loop(4, hot_left)
    loop(2, hot_here)
    write_held('wait')
    if not twin:
        loop(4, partner_left)
    loop(turns, turned_left)
    loop(16, home_left)
    loop(16, receive)


def hot_facts(hot_ref, flat):
    low, high = jnp.minimum(hot_ref[0], hot_ref[1]), jnp.maximum(hot_ref[0], hot_ref[1])
    at_low, at_high = low // HOME == flat, high // HOME == flat
    one = at_low != at_high
    hot_place = jnp.where(at_low, low, high) % HOME
    late_place = jnp.where(one, 1 - hot_place, 0)
    return low, high, one, late_place


DEPTH, LAG = 10, 5


def place_kernel(hot_ref, map_ref, gate, up, down, fused_home, down_home, hot,
                 fused_out, down_out, vm, zero, in_sem, out_sem):
    stage, core, y, x = coords()
    flat = stage * 2 + core
    late_stage = jnp.where(core == 0, y * 2 + (1 - x), (1 - y) * 2 + x)
    low, high, one_hot, late_place = hot_facts(hot_ref, flat)
    crossed = (hot_ref[0] > hot_ref[1]).astype(jnp.int32)
    zero[...] = jnp.zeros_like(zero)
    items = [(l, t) for t in range(SLOTS) for l in range(LAYERS)]

    def is_late(l, t):
        return jnp.logical_and(late_stage == l // 2, late_place == t)

    def inputs(k):
        l, t = items[k]
        b = k % DEPTH
        bf, bd = vm.at[b, pl.ds(0, HIDDEN)], vm.at[b, pl.ds(HIDDEN, WIDTH)]
        own = stage == l // 2
        if t < HOME:
            unit = flat * HOME + t
            hot_here = jnp.logical_or(unit == low, unit == high)
            h = (unit == high).astype(jnp.int32)
            direct = jnp.logical_and(own, core == y)
            other = jnp.logical_not(jnp.logical_or(direct, is_late(l, t)))
            place = jnp.where(one_hot, 1, t)
            arrived = [pltpu.make_async_copy(fused_home.at[l, place], bf, in_sem.at[b, 0]),
                       pltpu.make_async_copy(down_home.at[l, place], bd, in_sem.at[b, 1])]
            return [(direct, unit_reads(gate, up, down, l % 2, x * 4 + core * 2 + t, vm.at[b], in_sem.at[b])),
                    (jnp.logical_and(other, hot_here), [pltpu.make_async_copy(hot.at[h, l], vm.at[b], in_sem.at[b, 0])]),
                    (jnp.logical_and(other, jnp.logical_not(hot_here)), arrived)]
        v = map_ref[flat, t - HOME]
        used = v >= 0
        v = jnp.maximum(v, 0)
        unit = hot_ref[v]
        direct = jnp.logical_and(own, unit // LOCAL_EXPERTS == core)
        return [(jnp.logical_and(used, direct), unit_reads(gate, up, down, l % 2, unit % LOCAL_EXPERTS, vm.at[b], in_sem.at[b])),
                (jnp.logical_and(used, jnp.logical_not(direct)),
                 [pltpu.make_async_copy(hot.at[jnp.where(crossed == 1, 1 - v, v), l], vm.at[b], in_sem.at[b, 0])])]

    def outputs(k):
        l, t = items[k]
        b = k % DEPTH

        def put(src):
            return [pltpu.make_async_copy(src.at[pl.ds(0, HIDDEN)], fused_out.at[l, t], out_sem.at[b, 0]),
                    pltpu.make_async_copy(src.at[pl.ds(HIDDEN, WIDTH)], down_out.at[l, t], out_sem.at[b, 1])]
        if t < HOME:
            return [(jnp.logical_not(is_late(l, t)), put(vm.at[b]))]
        used = map_ref[flat, t - HOME] >= 0
        return [(used, put(vm.at[b])), (jnp.logical_not(used), put(zero))]

    def run(groups, verb):
        for cond, copies in groups:
            def act():
                for c in copies:
                    getattr(c, verb)()
            if cond is None:
                act()
            else:
                pl.when(cond)(act)

    n = len(items)
    for k in range(n + LAG):
        if k < n:
            if k >= DEPTH:
                run(outputs(k - DEPTH), 'wait')
            run(inputs(k), 'start')
        if k >= LAG:
            run(inputs(k - LAG), 'wait')
            run(outputs(k - LAG), 'start')
    for k in range(n - DEPTH, n):
        run(outputs(k), 'wait')


def late_layer(hot_ref):
    stage, core, y, x = coords()
    late_stage = jnp.where(core == 0, y * 2 + (1 - x), (1 - y) * 2 + x)
    return 2 * late_stage, hot_facts(hot_ref, stage * 2 + core)[-1]


def finish_kernel(hot_ref, late, fused_in, down_in, fused_out, down_out, vm, sem):
    del fused_in, down_in
    l, t = late_layer(hot_ref)
    dsts = (fused_out.at[l, t], down_out.at[l, t], fused_out.at[l + 1, t])
    parts = (pl.ds(0, HIDDEN), pl.ds(HIDDEN, WIDTH), pl.ds(ROWS, HIDDEN))
    reads = [pltpu.make_async_copy(late.at[p], vm.at[p], sem.at[0, k]) for k, p in enumerate(parts)]
    writes = [pltpu.make_async_copy(vm.at[p], dsts[k], sem.at[1, k]) for k, p in enumerate(parts)]
    for c in reads:
        c.start()
    for read, write in zip(reads, writes):
        read.wait()
        write.start()
    for c in writes:
        c.wait()


def close_kernel(hot_ref, last, down_in, down_out, sem):
    del down_in
    l, t = late_layer(hot_ref)
    write = pltpu.make_async_copy(last, down_out.at[l + 1, t], sem)
    write.start()
    write.wait()


def solution(mesh):
    flat_axes = ('stage', 'expert')
    S = jax.ShapeDtypeStruct
    home = (S((LAYERS, HOME, HIDDEN, 2 * WIDTH), BF16), S((LAYERS, HOME, WIDTH, HIDDEN), BF16))
    outs = (S((LAYERS, SLOTS, HIDDEN, 2 * WIDTH), BF16), S((LAYERS, SLOTS, WIDTH, HIDDEN), BF16))
    DMA = pltpu.SemaphoreType.DMA

    def exchange(homes):
        return pl.pallas_call(
            functools.partial(exchange_kernel, homes),
            out_shape=(*home, S((HOT, LAYERS, ROWS, HIDDEN), BF16), S((ROWS + HIDDEN, HIDDEN), BF16), S((WIDTH, HIDDEN), BF16),
                       S((4, ROWS, HIDDEN), BF16)),
            in_specs=[SMEM] + [ANY] * 3, out_specs=(ANY,) * 6,
            scratch_shapes=[DMA((16,)), DMA((4, 2, 2)), DMA((HOT, 2, 3)), DMA((HOT, 2, 3)), DMA((HOT,)), DMA((HOT, 2)), DMA((4,)), DMA((4,)),
                            pltpu.VMEM((HOT, LOCAL_LAYERS, 2, ROWS, HIDDEN), BF16), DMA((HOT,)),
                            pltpu.VMEM((LOCAL_LAYERS, ROWS, HIDDEN), BF16), DMA((LOCAL_LAYERS, 4)), DMA],
            compiler_params=pltpu.CompilerParams(has_side_effects=True, vmem_limit_bytes=66_900_000))

    place = pl.pallas_call(
        place_kernel, out_shape=outs, in_specs=[SMEM, SMEM] + [ANY] * 6, out_specs=(ANY, ANY),
        scratch_shapes=[pltpu.VMEM((DEPTH, ROWS, HIDDEN), BF16), pltpu.VMEM((ROWS, HIDDEN), BF16), DMA((DEPTH, 3)), DMA((DEPTH, 2))],
        cost_estimate=pl.CostEstimate(flops=10 ** 9, bytes_accessed=2 * 10 ** 8, transcendentals=0),
        compiler_params=pltpu.CompilerParams(vmem_limit_bytes=48 * 1024 * 1024))

    finish = pl.pallas_call(
        finish_kernel, out_shape=outs, in_specs=[SMEM] + [ANY] * 3, out_specs=(ANY, ANY), input_output_aliases={2: 0, 3: 1},
        scratch_shapes=[pltpu.VMEM((ROWS + HIDDEN, HIDDEN), BF16), DMA((2, 3))],
        compiler_params=pltpu.CompilerParams(vmem_limit_bytes=16 * 1024 * 1024))

    close = pl.pallas_call(
        close_kernel, out_shape=outs[1], in_specs=[SMEM, pl.BlockSpec(memory_space=pltpu.VMEM), ANY], out_specs=ANY,
        input_output_aliases={2: 0}, scratch_shapes=[DMA],
        compiler_params=pltpu.CompilerParams(vmem_limit_bytes=4 * 1024 * 1024))

    pairs = []
    for y in range(2):
        for x in range(2):
            pairs.append(((y * 2 + x) * 2 + y, (y * 2 + 1 - x) * 2))
            pairs.append(((y * 2 + x) * 2 + 1 - y, ((1 - y) * 2 + x) * 2 + 1))

    def local(gate, up, down, hot_units, slot_map):
        homes = hot_units // HOME
        low, high = jnp.min(homes), jnp.max(homes)
        fused_home, down_home, hot, late, last, _ = lax.switch(
            high * (high + 1) // 2 + low, [exchange(p) for p in PAIRS], hot_units, gate, up, down)
        late = lax.ppermute(late, flat_axes, pairs)
        last = lax.ppermute(last, flat_axes, pairs)
        fused, down_out = place(hot_units, slot_map, gate, up, down, fused_home, down_home, hot)
        fused, down_out = finish(hot_units, late, fused, down_out)
        return fused, close(hot_units, last, down_out)

    return jax.shard_map(local, mesh=mesh, in_specs=(P('stage', 'expert'), P('stage', 'expert'), P('stage', 'expert'), P(), P()),
                         out_specs=(P(None, flat_axes), P(None, flat_axes)), check_vma=False)
```
